32 devices in a mesh: tm: 8 (over z, core), bank: 4 (over y, x).
Axes of the slice: x: 2, y: 2, z: 4, core: 2. Of those that a mesh axis runs over, the one named last changes fastest.
Arguments:
- strain: float32 [16, 131072], P('tm', 'bank'), may hold values from -40 to 40
- lengths: int32 [16], P('tm'), may hold values from 65536 to 131072
- templates: bfloat16 [2, 16, 512, 512], P(None, 'bank'), may hold values from -6 to 6
Outputs:
- snr: float32 [16, 2097152], P('bank', 'tm')
The draws below stay inside these ranges and needn't reach their ends.
All inputs are finite; a program needn't handle non-finite values.
Results may differ from the reference program's by a relative error of at most 0.014.
Values may be sent and summed in bfloat16 or wider, within the bound.
No kernel may reach another device: no remote copies, remote signals or barrier semaphores. Data moves between devices by JAX's collectives and lax.ppermute only.
A program may use at most 128 MiB of HBM per device.

```python
import math
import jax
import jax.numpy as jnp
from jax import lax

R = 512
BLOCK = 131072
BLOCKS = 16
NTEMP = 16


line_count = 64


def draw_strain(key, part):
    noise_key, freq_key, phase_key, amp_key = jax.random.split(jax.random.fold_in(key, 7), 4)
    position = jnp.arange(BLOCKS * BLOCK, dtype=jnp.float32).reshape(BLOCKS, BLOCK)
    fraction = position / (BLOCKS * BLOCK)
    noise = jax.random.truncated_normal(noise_key, -6.0, 6.0, (BLOCKS, BLOCK), jnp.float32)
    envelope = 1.0 + 2.0 * fraction
    freqs = jax.random.uniform(freq_key, (line_count,), jnp.float32, 0.01, 0.49)
    phases = jax.random.uniform(phase_key, (line_count,), jnp.float32, 0.0, 2.0 * math.pi)
    amplitudes = jnp.exp(jax.random.uniform(amp_key, (line_count,), jnp.float32, math.log(0.01), math.log(0.3)))

    def add_line(total, item):
        frequency, phase, amplitude = item
        cycles = jnp.mod(frequency * position, 1.0)
        return (total + amplitude * jnp.cos(2.0 * math.pi * cycles + phase), None)
    lines, unused = lax.scan(add_line, jnp.zeros((BLOCKS, BLOCK), jnp.float32), (freqs, phases, amplitudes))
    return noise * envelope + lines


def touch_ends(array, own_key, smallest, largest):
    longest = array.shape.index(max(array.shape))
    spots = []
    for shift in (0, 1):
        where = [jax.random.randint(jax.random.fold_in(own_key, axis), (), 0, length) for axis, length in enumerate(array.shape)]
        where[longest] = (where[longest] + shift) % array.shape[longest]
        spots.append(tuple(where))
    return array.at[spots[0]].set(smallest).at[spots[1]].set(largest)


def shard_levels(rng, extent, shards, low, top_value):
    loudness = 1.0
    for dim, blocks in shards:
        steps = jax.random.uniform(jax.random.fold_in(jax.random.fold_in(rng, 6), dim), (blocks,), jnp.float32, low / len(shards), top_value / len(shards))
        loudness = loudness * jnp.repeat(jnp.exp(steps), extent[dim] // blocks).reshape((-1,) + (1,) * (len(extent) - 1 - dim))
    return loudness


def gaussian(own_key, extent, spread, most, shards=(), kind=jnp.bfloat16):
    array = jax.random.normal(own_key, extent, jnp.float32) * spread
    if len(shards) > 0:
        array = shard_levels(own_key, extent, shards, -0.22, 0.18) * array
    return jnp.clip(array, min=-most, max=most).astype(kind)


def setup_inputs(seed: int = 0) -> dict:
    key_of = jax.random.split(jax.random.key(seed), 4)
    strain = draw_strain(jax.random.fold_in(key_of[3], 71), 0)
    lengths = touch_ends(jax.random.randint(key_of[1], (BLOCKS,), BLOCK // 2, BLOCK + 1), jax.random.fold_in(key_of[1], 1), BLOCK // 2, BLOCK).astype(jnp.int32)
    templates = gaussian(key_of[2], (2, NTEMP, R, R), 1.0, 6.0, ((1, 4),))
    return {"strain": strain, "lengths": lengths, "templates": templates}


epsilon = 1e-06
two_pi = 2.0 * math.pi

def dft_tables(order):
    index = jnp.arange(order, dtype=jnp.int32)
    product = index[:, None] * index[None, :]
    angle = (product % order).astype(jnp.float32) * (two_pi / order)
    twist = product.astype(jnp.float32) * (two_pi / (order * order))
    return (jnp.cos(angle).astype(jnp.bfloat16), jnp.sin(angle).astype(jnp.bfloat16), jnp.cos(twist), jnp.sin(twist))

def rounded(values):
    return lax.optimization_barrier(values.astype(jnp.bfloat16)).astype(jnp.float32)

def reference(strain, lengths, templates):
    cosine, sine, twist_cos, twist_sin = dft_tables(R)
    cos_full = cosine.astype(jnp.float32)
    sin_full = sine.astype(jnp.float32)
    half_rows = R // 2
    position = jnp.arange(BLOCK, dtype=jnp.int32)
    valid = position[None, :] < lengths[:, None]
    gated = rounded(jnp.where(valid, strain, 0.0)).reshape(BLOCKS, half_rows, R)
    first_real = jnp.einsum('kn,cnm->ckm', cos_full[:, :half_rows], gated)
    first_imag = -jnp.einsum('kn,cnm->ckm', sin_full[:, :half_rows], gated)
    twist_real = rounded(first_real * twist_cos + first_imag * twist_sin)
    twist_imag = rounded(first_imag * twist_cos - first_real * twist_sin)
    spec_real = jnp.einsum('ckn,nm->ckm', twist_real, cos_full) + jnp.einsum('ckn,nm->ckm', twist_imag, sin_full)
    spec_imag = jnp.einsum('ckn,nm->ckm', twist_imag, cos_full) - jnp.einsum('ckn,nm->ckm', twist_real, sin_full)
    power = lax.optimization_barrier(jnp.sum(spec_real * spec_real + spec_imag * spec_imag, axis=0))
    weight = lax.rsqrt(power / BLOCKS + epsilon)
    white_real = rounded(spec_real * weight)
    white_imag = rounded(spec_imag * weight)

    def filter_one(template_pair):
        tmpl_real = template_pair[0].astype(jnp.float32)
        tmpl_imag = template_pair[1].astype(jnp.float32)
        prod_real = rounded(tmpl_real * white_real + tmpl_imag * white_imag)
        prod_imag = rounded(tmpl_real * white_imag - tmpl_imag * white_real)
        inner_real = jnp.einsum('ckm,mn->ckn', prod_real, cos_full) - jnp.einsum('ckm,mn->ckn', prod_imag, sin_full)
        inner_imag = jnp.einsum('ckm,mn->ckn', prod_real, sin_full) + jnp.einsum('ckm,mn->ckn', prod_imag, cos_full)
        back_real = rounded(inner_real * twist_cos - inner_imag * twist_sin)
        back_imag = rounded(inner_imag * twist_cos + inner_real * twist_sin)
        output = jnp.einsum('nk,ckm->cnm', cos_full, back_real) - jnp.einsum('nk,ckm->cnm', sin_full, back_imag)
        factor = lax.rsqrt(jnp.sum(tmpl_real * tmpl_real + tmpl_imag * tmpl_imag))
        flat = output.reshape(BLOCKS, R * R)
        own_part = flat[:, :BLOCK] * factor
        tail_part = flat[:, BLOCK:] * factor
        previous = jnp.concatenate([jnp.zeros((1, BLOCK), own_part.dtype), tail_part[:-1]], axis=0)
        return (own_part + previous).reshape(BLOCKS * BLOCK)
    moved = jnp.moveaxis(templates, 1, 0)
    return lax.map(filter_one, moved)
```

```python
import functools
import math

import jax
import jax.numpy as jnp
import numpy as np
from jax import lax
from jax.experimental import pallas as pl
from jax.experimental.pallas import tpu as pltpu
from jax.sharding import PartitionSpec as P

epsilon = 1e-06
bf16 = jnp.bfloat16
f32 = jnp.float32


def dot(a, b):
    return jnp.dot(a, b, preferred_element_type=f32)


def tables(order):
    half = order // 2
    rows = half + 16
    a = np.arange(rows)
    keep = (a <= half)[:, None]
    turn = 2.0 * math.pi / order

    def angle(left, right):
        return turn * ((left[:, None] * right[None, :]) % order)

    u, v = np.arange(half), np.arange(order)
    first = np.concatenate([np.cos(angle(a, u)) * keep, -np.sin(angle(a, u)) * keep])
    twist = (2.0 * math.pi / order**2) * (a[:, None] * v[None, :])
    even, odd = angle(u, 2 * u), angle(u, 2 * u + 1)
    sections = [np.cos(even), np.sin(even), np.cos(odd), np.sin(odd), np.cos(odd).T, np.sin(odd).T]
    last_cos, last_sin = np.cos(angle(u, u)), -np.sin(angle(u, u))
    last_cos[:, 0] = 0.5
    last_sin[:, 0] = 0.5 * (1.0 - 2.0 * (u % 2))
    return dict(
        first=first.astype(bf16),
        twist=np.stack([np.cos(twist), np.sin(twist)]).astype(np.float32),
        sections=np.stack(sections).astype(bf16),
        last=np.concatenate([last_cos, last_sin], axis=1).astype(bf16),
    )


def fill_sections(dest, cosine, sine, sign):
    half = cosine.shape[0]
    positive, negative = (sine, -sine) if sign > 0 else (-sine, sine)
    dest[:half, :half] = cosine
    dest[:half, half:] = positive
    dest[half:, :half] = negative
    dest[half:, half:] = cosine


def spectrum(samples, first, twist, even_table, odd_table):
    rows = first.shape[0] // 2
    half = first.shape[1]
    out = dot(first[...], samples)
    real, imag = out[:rows], out[rows:]
    tc, ts = twist[0], twist[1]
    tr = real * tc + imag * ts
    ti = imag * tc - real * ts
    plus = jnp.concatenate([tr[:, :half] + tr[:, half:], ti[:, :half] + ti[:, half:]], axis=1)
    minus = jnp.concatenate([tr[:, :half] - tr[:, half:], ti[:, :half] - ti[:, half:]], axis=1)
    return dot(plus.astype(bf16), even_table[...]), dot(minus.astype(bf16), odd_table[...])


def alternate(values):
    row = lax.broadcasted_iota(jnp.int32, values.shape, 0)
    return jnp.where(row % 2 == 0, values, -values)


def spectrum_kernel(
    place, *refs, shards
):
    pieces = refs[:shards]
    first, twist, sections = refs[shards : shards + 3]
    kept, summed, power, last_block, samples, even_table, odd_table = refs[shards + 3 :]
    rows = first.shape[0] // 2
    half = first.shape[1]
    piece_rows = pieces[0].shape[1]
    for s in range(shards):
        at = pl.multiple_of((place[0] ^ s) * piece_rows, piece_rows)
        samples[:, pl.ds(at, piece_rows), :] = pieces[s][...]
    fill_sections(even_table, sections[0], sections[1], -1)
    fill_sections(odd_table, sections[2], sections[3], -1)
    last_block[...] = samples[1]
    even0, odd0 = spectrum(samples[0], first, twist, even_table, odd_table)
    even1, odd1 = spectrum(samples[1], first, twist, even_table, odd_table)
    for side, (one, two) in enumerate(((even0, even1), (odd0, odd1))):
        at = side * half
        for part in range(2):
            x0 = one[:, part * half : (part + 1) * half]
            x1 = two[:, part * half : (part + 1) * half]
            kept[part, :, at : at + half] = x0
            summed[part, :, at : at + half] = x1 + alternate(x0)
        total = (
            one[:, :half] * one[:, :half]
            + one[:, half:] * one[:, half:]
            + two[:, :half] * two[:, :half]
            + two[:, half:] * two[:, half:]
        )
        for lane in range(half // 128):
            row = (side * (half // 128) + lane) * rows
            power[row : row + rows, :] = total[:, lane * 128 : (lane + 1) * 128].astype(bf16)


def previous_kernel(samples, kept, first, twist, sections, summed, even_table, odd_table):
    half = first.shape[1]
    fill_sections(even_table, sections[0], sections[1], -1)
    fill_sections(odd_table, sections[2], sections[3], -1)
    sides = spectrum(samples[...], first, twist, even_table, odd_table)
    for side in range(2):
        at = side * half
        for part in range(2):
            x = sides[side][:, part * half : (part + 1) * half]
            summed[part, :, at : at + half] = kept[part, :, at : at + half] + alternate(x)


def template_kernel(templates, folded, factor):
    order = templates.shape[-1]
    half = order // 2
    quarter = half // 2
    rows = folded.shape[2]
    a = lax.broadcasted_iota(jnp.int32, (rows, half), 0)
    r = lax.broadcasted_iota(jnp.int32, (rows, half), 1)
    flip = jnp.where((r == half - a) & (a >= 1), 1.0, 0.0).astype(bf16)
    m = lax.broadcasted_iota(jnp.int32, (half, half), 0)
    q = lax.broadcasted_iota(jnp.int32, (half, half), 1)
    source = jnp.where(q < quarter, 2 * q, 2 * (q - quarter) + 1)
    order_up = jnp.where(m == source, 1.0, 0.0).astype(bf16)
    order_down = jnp.where(m == half - 1 - source, 1.0, 0.0).astype(bf16)
    top_row = lax.broadcasted_iota(jnp.int32, (8, half), 0) == 0
    energy = jnp.zeros((8, order), f32)
    for part in range(2):
        whole = templates[part, 0]
        square = whole.astype(f32) * whole.astype(f32)
        energy = energy + jnp.sum(square.reshape(order // 8, 8, order), axis=0)
        upper = whole[:rows]
        lower = dot(flip, whole[half:])
        first = lax.broadcasted_iota(jnp.int32, (rows, order), 0) == 0
        lower = jnp.where(first, whole[0:1].astype(f32), lower).astype(bf16)
        up = [dot(upper[:, :half], order_up), dot(upper[:, half:], order_up)]
        down = [dot(lower[:, half:], order_down), dot(lower[:, :half], order_down)]

        def sides(pair):
            return [
                jnp.concatenate([pair[0][:, at : at + quarter], pair[1][:, at : at + quarter]], axis=1)
                for at in (0, quarter)
            ]

        up_even, up_odd = sides(up)
        down_even, down_odd = sides(down)
        fixed_even = jnp.where(top_row, pltpu.roll(down_odd[:8], 1, 1), down_even[:8])
        fixed_odd = jnp.where(top_row, down_even[:8], down_odd[:8])
        down_even = jnp.concatenate([fixed_even, down_even[8:]], axis=0)
        down_odd = jnp.concatenate([fixed_odd, down_odd[8:]], axis=0)
        sign = 1.0 if part == 0 else -1.0
        folded[0, part, :, :half] = (up_even + sign * down_even).astype(bf16)
        folded[0, part, :, half:] = (up_odd + sign * down_odd).astype(bf16)
    total = jnp.sum(jnp.sum(energy, axis=1, keepdims=True), axis=0, keepdims=True)
    factor[0] = jnp.broadcast_to(lax.rsqrt(total), factor.shape[1:])


def filter_kernel(
    place, mine, theirs, earlier, later, folded, factor, twist, sections, last, out,
    weight, white, even_table, odd_table, back, *, blocks
):
    half = last.shape[0]
    rows = twist.shape[1]
    count = pl.num_programs(1)
    block, template = pl.program_id(0), pl.program_id(1)

    @pl.when((block == 0) & (template == 0))
    def _():
        fill_sections(even_table, sections[0], sections[1], 1)
        fill_sections(odd_table, sections[4], sections[5], 1)
        chunk = mine.shape[1]
        for s in range(mine.shape[0]):
            for pieces, core in ((mine, place[1]), (theirs, 1 - place[1])):
                at = pl.multiple_of(((place[0] ^ s) * 2 + core) * chunk, 8)
                total = pieces[s].astype(f32)
                weight[pl.ds(at, chunk), :] = lax.rsqrt(total / blocks + epsilon)

    def whiten(spectra):
        for part in range(2):
            for lane in range(2 * half // 128):
                cols = slice(lane * 128, (lane + 1) * 128)
                white[part, :, cols] = spectra[part, :, cols] * weight[lane * rows : (lane + 1) * rows, :]

    @pl.when((block == 0) & (template == 0))
    def _():
        whiten(earlier)

    @pl.when((block == 1) & (template == 0))
    def _():
        whiten(later)

    vr, vi = white[0], white[1]
    gr, gi = folded[0, 0].astype(f32), folded[0, 1].astype(f32)
    pr = (gr * vr + gi * vi).astype(bf16)
    pi = (gr * vi - gi * vr).astype(bf16)
    even = dot(jnp.concatenate([pr[:, :half], pi[:, :half]], axis=1), even_table[...])
    odd = dot(jnp.concatenate([pr[:, half:], pi[:, half:]], axis=1), odd_table[...])
    er, ei, orr, oi = even[:, :half], even[:, half:], odd[:, :half], odd[:, half:]
    for side, (ir, ii) in enumerate(((er + orr, ei + oi), (er - orr, ei - oi))):
        cols = slice(side * half, (side + 1) * half)
        tc, ts = twist[0, :, cols], twist[1, :, cols]
        br = ir * tc - ii * ts
        bi = ii * tc + ir * ts
        back[:half, cols] = br[:half].astype(bf16)
        back[half:, cols] = bi[:half].astype(bf16)
        first = lax.broadcasted_iota(jnp.int32, (16, half), 0) == 0
        back[half : half + 16, cols] = jnp.where(first, br[half : half + 1], bi[:16]).astype(bf16)
    scale = factor[0, 0:1, :]
    result = dot(last[...], back[...])
    lanes = 2 * half // 128
    for lane in range(lanes):
        piece = result[:, lane * 128 : (lane + 1) * 128] * scale
        out[pl.ds(lane * count + template, half, stride=lanes * count), :] = piece


def exchange(values, axis, pairs_of):
    size = lax.axis_size(axis)
    return lax.ppermute(values, axis, [(i, pairs_of(i)) for i in range(size)])


def body(strain, lengths, templates):
    blocks_here, local = strain.shape
    count, order = templates.shape[1], templates.shape[-1]
    half = order // 2
    rows = half + 16
    banks, groups = lax.axis_size("bank"), lax.axis_size("tm")
    bank, group = lax.axis_index("bank"), lax.axis_index("tm")
    core = group % 2
    place = jnp.stack([bank, core]).astype(jnp.int32)
    table = tables(order)
    vmem = pl.BlockSpec(memory_space=pltpu.VMEM)
    smem = pl.BlockSpec(memory_space=pltpu.SMEM)
    limit = pltpu.CompilerParams(vmem_limit_bytes=60 * 1024 * 1024)

    index = bank * local + jnp.arange(local, dtype=jnp.int32)
    valid = index[None, :] < lengths[:, None]
    gated = jnp.where(valid, strain, 0.0).astype(bf16).reshape(blocks_here, local // order, order)
    pieces = [gated] + [exchange(gated, "bank", lambda i, s=s: i ^ s) for s in range(1, banks)]

    folded, factor = pl.pallas_call(
        template_kernel,
        grid=(count,),
        in_specs=[pl.BlockSpec((2, 1, order, order), lambda t: (0, t, 0, 0))],
        out_specs=[
            pl.BlockSpec((1, 2, rows, order), lambda t: (t, 0, 0, 0)),
            pl.BlockSpec((1, 8, 128), lambda t: (t, 0, 0)),
        ],
        out_shape=[
            jax.ShapeDtypeStruct((count, 2, rows, order), bf16),
            jax.ShapeDtypeStruct((count, 8, 128), f32),
        ],
        cost_estimate=pl.CostEstimate(flops=int(6e9), bytes_accessed=int(6.5e6), transcendentals=0),
        compiler_params=limit,
        name="fold_templates",
    )(templates)

    plane = jax.ShapeDtypeStruct((2, rows, order), f32)
    square = pltpu.VMEM((order, order), bf16)
    kept, later, power, last_block = pl.pallas_call(
        functools.partial(spectrum_kernel, shards=banks),
        in_specs=[smem] + [vmem] * (banks + 3),
        out_specs=[vmem] * 4,
        out_shape=[
            plane,
            plane,
            jax.ShapeDtypeStruct((rows * order // 128, 128), bf16),
            jax.ShapeDtypeStruct((half, order), bf16),
        ],
        scratch_shapes=[pltpu.VMEM((blocks_here, half, order), bf16), square, square],
        cost_estimate=pl.CostEstimate(flops=int(2e9), bytes_accessed=int(5e6), transcendentals=0),
        compiler_params=limit,
        name="spectra",
    )(place, *pieces, table["first"], table["twist"], table["sections"])

    chunk = power.shape[0] // (2 * banks)
    own_part = lax.dynamic_index_in_dim(power.reshape(banks, 2, chunk, 128), bank, 0, False)
    mine = lax.dynamic_index_in_dim(own_part, core, 0, False)
    other = lax.dynamic_index_in_dim(own_part, 1 - core, 0, False)
    partner = exchange(other, "tm", lambda i: i ^ 1)
    chip = (mine.astype(f32) + partner.astype(f32)).astype(bf16)
    share = chip.astype(f32)
    for step in range(1, groups // 2):
        share = share + exchange(chip, "tm", lambda i, s=step: i ^ (2 * s)).astype(f32)
    share = share.astype(bf16)
    last_block, share = lax.optimization_barrier((last_block, share))
    mine = jnp.stack([share] + [exchange(share, "bank", lambda i, s=s: i ^ s) for s in range(1, banks)])
    theirs = exchange(mine, "tm", lambda i: i ^ 1)

    before = lax.ppermute(last_block, "tm", [(i, i + 1) for i in range(groups - 1)])
    earlier = pl.pallas_call(
        previous_kernel,
        in_specs=[vmem] * 5,
        out_specs=vmem,
        out_shape=plane,
        scratch_shapes=[square, square],
        cost_estimate=pl.CostEstimate(flops=int(1e9), bytes_accessed=int(4e6), transcendentals=0),
        compiler_params=limit,
        name="previous",
    )(before, kept, table["first"], table["twist"], table["sections"])

    lines = count * half * order // 128
    out = pl.pallas_call(
        functools.partial(filter_kernel, blocks=float(blocks_here * groups)),
        grid=(blocks_here, count),
        in_specs=[smem, vmem, vmem, vmem, vmem]
        + [
            pl.BlockSpec((1, 2, rows, order), lambda c, t: (t, 0, 0, 0)),
            pl.BlockSpec((1, 8, 128), lambda c, t: (t, 0, 0)),
        ]
        + [vmem] * 3,
        out_specs=pl.BlockSpec((lines, 128), lambda c, t: (c, 0)),
        out_shape=jax.ShapeDtypeStruct((blocks_here * lines, 128), f32),
        scratch_shapes=[
            pltpu.VMEM((rows * order // 128, 128), f32),
            pltpu.VMEM((2, rows, order), f32),
            square,
            square,
            square,
        ],
        cost_estimate=pl.CostEstimate(flops=int(6e9), bytes_accessed=int(1.2e7), transcendentals=0),
        compiler_params=limit,
        name="filter",
    )(place, mine, theirs, earlier, later, folded, factor, table["twist"], table["sections"], table["last"])
    split = out.reshape(blocks_here * half * order // 128, count, 128)
    return jnp.swapaxes(split, 0, 1).reshape(count, blocks_here * half * order)


def solution(mesh):
    in_specs = (P("tm", "bank"), P("tm"), P(None, "bank", None, None))
    out_specs = P("bank", "tm")
    return jax.shard_map(body, mesh=mesh, in_specs=in_specs, out_specs=out_specs, check_vma=False)
```

```python
import functools
import math

import jax
import jax.numpy as jnp
import numpy as np
from jax import lax
from jax.experimental import pallas as pl
from jax.experimental.pallas import tpu as pltpu
from jax.sharding import PartitionSpec as P

epsilon = 1e-06
bf16 = jnp.bfloat16
f32 = jnp.float32


def dot(a, b):
    return jnp.dot(a, b, preferred_element_type=f32)


def tables(order):
    half = order // 2
    rows = half + 16
    a = np.arange(rows)
    keep = (a <= half)[:, None]
    turn = 2.0 * math.pi / order

    def angle(left, right):
        return turn * ((left[:, None] * right[None, :]) % order)

    u, v = np.arange(half), np.arange(order)
    first = np.concatenate([np.cos(angle(a, u)) * keep, -np.sin(angle(a, u)) * keep])
    twist = (2.0 * math.pi / order**2) * (a[:, None] * v[None, :])
    even, odd = angle(u, 2 * u), angle(u, 2 * u + 1)
    sections = [np.cos(even), np.sin(even), np.cos(odd), np.sin(odd), np.cos(odd).T, np.sin(odd).T]
    last_cos, last_sin = np.cos(angle(u, u)), -np.sin(angle(u, u))
    last_cos[:, 0] = 0.5
    last_sin[:, 0] = 0.5 * (1.0 - 2.0 * (u % 2))
    return dict(
        first=first.astype(bf16),
        twist=np.stack([np.cos(twist), np.sin(twist)]).astype(np.float32),
        sections=np.stack(sections).astype(bf16),
        last=np.concatenate([last_cos, last_sin], axis=1).astype(bf16),
    )


def fill_sections(dest, cosine, sine, sign):
    half = cosine.shape[0]
    positive, negative = (sine, -sine) if sign > 0 else (-sine, sine)
    dest[:half, :half] = cosine
    dest[:half, half:] = positive
    dest[half:, :half] = negative
    dest[half:, half:] = cosine


def spectrum(samples, first, twist, even_table, odd_table):
    rows = first.shape[0] // 2
    half = first.shape[1]
    out = dot(first[...], samples)
    real, imag = out[:rows], out[rows:]
    tc, ts = twist[0], twist[1]
    tr = real * tc + imag * ts
    ti = imag * tc - real * ts
    plus = jnp.concatenate([tr[:, :half] + tr[:, half:], ti[:, :half] + ti[:, half:]], axis=1)
    minus = jnp.concatenate([tr[:, :half] - tr[:, half:], ti[:, :half] - ti[:, half:]], axis=1)
    return dot(plus.astype(bf16), even_table[...]), dot(minus.astype(bf16), odd_table[...])


def alternate(values):
    row = lax.broadcasted_iota(jnp.int32, values.shape, 0)
    return jnp.where(row % 2 == 0, values, -values)


def spectrum_kernel(*refs, shards):
    pieces = refs[:shards]
    first, twist, sections = refs[shards : shards + 3]
    kept, summed, mine, other, last_block, samples, power, even_table, odd_table = refs[shards + 3 :]
    rows = first.shape[0] // 2
    half = first.shape[1]
    piece_rows = pieces[0].shape[1]
    bank, core = lax.axis_index("bank"), lax.rem(lax.axis_index("tm"), 2)
    for s in range(shards):
        at = pl.multiple_of((bank ^ s) * piece_rows, piece_rows)
        samples[:, pl.ds(at, piece_rows), :] = pieces[s][...]
    fill_sections(even_table, sections[0], sections[1], -1)
    fill_sections(odd_table, sections[2], sections[3], -1)
    last_block[...] = samples[1]
    even0, odd0 = spectrum(samples[0], first, twist, even_table, odd_table)
    even1, odd1 = spectrum(samples[1], first, twist, even_table, odd_table)
    for side, (one, two) in enumerate(((even0, even1), (odd0, odd1))):
        at = side * half
        for part in range(2):
            x0 = one[:, part * half : (part + 1) * half]
            x1 = two[:, part * half : (part + 1) * half]
            kept[part, :, at : at + half] = x0.astype(bf16)
            summed[part, :, at : at + half] = (x1 + alternate(x0)).astype(bf16)
        total = (
            one[:, :half] * one[:, :half]
            + one[:, half:] * one[:, half:]
            + two[:, :half] * two[:, :half]
            + two[:, half:] * two[:, half:]
        )
        for lane in range(half // 128):
            row = (side * (half // 128) + lane) * rows
            power[row : row + rows, :] = total[:, lane * 128 : (lane + 1) * 128]
    chunk = mine.shape[0]
    for dest, which in ((mine, core), (other, 1 - core)):
        at = pl.multiple_of((bank * 2 + which) * chunk, 8)
        dest[...] = power[pl.ds(at, chunk), :].astype(bf16)


def previous_kernel(samples, kept, first, twist, sections, summed, even_table, odd_table):
    half = first.shape[1]
    fill_sections(even_table, sections[0], sections[1], -1)
    fill_sections(odd_table, sections[2], sections[3], -1)
    sides = spectrum(samples[...], first, twist, even_table, odd_table)
    for side in range(2):
        at = side * half
        for part in range(2):
            x = sides[side][:, part * half : (part + 1) * half]
            x = kept[part, :, at : at + half].astype(f32) + alternate(x)
            summed[part, :, at : at + half] = x.astype(bf16)


def template_kernel(templates, folded, factor):
    order = templates.shape[-1]
    half = order // 2
    quarter = half // 2
    rows = folded.shape[2]
    a = lax.broadcasted_iota(jnp.int32, (rows, half), 0)
    r = lax.broadcasted_iota(jnp.int32, (rows, half), 1)
    flip = jnp.where((r == half - a) & (a >= 1), 1.0, 0.0).astype(bf16)
    m = lax.broadcasted_iota(jnp.int32, (half, half), 0)
    q = lax.broadcasted_iota(jnp.int32, (half, half), 1)
    source = jnp.where(q < quarter, 2 * q, 2 * (q - quarter) + 1)
    order_up = jnp.where(m == source, 1.0, 0.0).astype(bf16)
    order_down = jnp.where(m == half - 1 - source, 1.0, 0.0).astype(bf16)
    top_row = lax.broadcasted_iota(jnp.int32, (8, half), 0) == 0
    energy = jnp.zeros((8, order), f32)
    for part in range(2):
        whole = templates[part, 0]
        square = whole.astype(f32) * whole.astype(f32)
        energy = energy + jnp.sum(square.reshape(order // 8, 8, order), axis=0)
        upper = whole[:rows]
        lower = dot(flip, whole[half:])
        first = lax.broadcasted_iota(jnp.int32, (rows, order), 0) == 0
        lower = jnp.where(first, whole[0:1].astype(f32), lower).astype(bf16)
        up = [dot(upper[:, :half], order_up), dot(upper[:, half:], order_up)]
        down = [dot(lower[:, half:], order_down), dot(lower[:, :half], order_down)]

        def sides(pair):
            return [
                jnp.concatenate([pair[0][:, at : at + quarter], pair[1][:, at : at + quarter]], axis=1)
                for at in (0, quarter)
            ]

        up_even, up_odd = sides(up)
        down_even, down_odd = sides(down)
        fixed_even = jnp.where(top_row, pltpu.roll(down_odd[:8], 1, 1), down_even[:8])
        fixed_odd = jnp.where(top_row, down_even[:8], down_odd[:8])
        down_even = jnp.concatenate([fixed_even, down_even[8:]], axis=0)
        down_odd = jnp.concatenate([fixed_odd, down_odd[8:]], axis=0)
        sign = 1.0 if part == 0 else -1.0
        folded[0, part, :, :half] = (up_even + sign * down_even).astype(bf16)
        folded[0, part, :, half:] = (up_odd + sign * down_odd).astype(bf16)
    total = jnp.sum(jnp.sum(energy, axis=1, keepdims=True), axis=0, keepdims=True)
    factor[0] = jnp.broadcast_to(lax.rsqrt(total), factor.shape[1:])


def filter_kernel(
    mine, theirs, earlier, later, folded, factor, twist, sections, last, out,
    weight, white, even_table, odd_table, back, result, sems, *, blocks
):
    half = last.shape[0]
    rows = twist.shape[1]
    count = folded.shape[0]
    lanes = 2 * half // 128
    fill_sections(even_table, sections[0], sections[1], 1)
    fill_sections(odd_table, sections[4], sections[5], 1)
    chunk = mine.shape[1]
    bank, own = lax.axis_index("bank"), lax.rem(lax.axis_index("tm"), 2)
    for s in range(mine.shape[0]):
        for pieces, core in ((mine, own), (theirs, 1 - own)):
            at = pl.multiple_of(((bank ^ s) * 2 + core) * chunk, 8)
            total = pieces[s].astype(f32)
            weight[pl.ds(at, chunk), :] = lax.rsqrt(total / blocks + epsilon)

    def copies(block, template):
        slot = block * count + template
        return [
            pltpu.make_async_copy(
                result.at[slot, :, pl.ds(lane * 128, 128)],
                out.at[pl.ds(block * half, half), lane * count + template, 0, :],
                sems.at[slot],
            )
            for lane in range(lanes)
        ]

    for block, spectra in enumerate((earlier, later)):
        for part in range(2):
            for lane in range(lanes):
                cols = slice(lane * 128, (lane + 1) * 128)
                scaled = spectra[part, :, cols].astype(f32) * weight[lane * rows : (lane + 1) * rows, :]
                white[block, part, :, cols] = scaled.astype(bf16)
        for template in range(count):
            slot = block * count + template
            vr, vi = white[block, 0], white[block, 1]
            gr, gi = folded[template, 0], folded[template, 1]
            pr = gr * vr + gi * vi
            pi = gr * vi - gi * vr
            even = dot(jnp.concatenate([pr[:, :half], pi[:, :half]], axis=1), even_table[...]).astype(bf16)
            odd = dot(jnp.concatenate([pr[:, half:], pi[:, half:]], axis=1), odd_table[...]).astype(bf16)
            er, ei, orr, oi = even[:, :half], even[:, half:], odd[:, :half], odd[:, half:]
            for side, (ir, ii) in enumerate(((er + orr, ei + oi), (er - orr, ei - oi))):
                cols = slice(side * half, (side + 1) * half)
                tc, ts = twist[0, :, cols].astype(bf16), twist[1, :, cols].astype(bf16)
                br = ir * tc - ii * ts
                bi = ii * tc + ir * ts
                back[slot, :half, cols] = br[:half]
                back[slot, half:, cols] = bi[:half]
                first = lax.broadcasted_iota(jnp.int32, (16, half), 0) == 0
                middle = jnp.broadcast_to(br[half : half + 1].astype(f32), (16, half))
                back[slot, half : half + 16, cols] = jnp.where(first, middle, bi[:16].astype(f32)).astype(bf16)
            scale = factor[template, 0:1, 0:1]
            result[slot] = dot(last[...], back[slot]) * scale
            for copy in copies(block, template):
                copy.start()
    for block in range(2):
        for template in range(count):
            for copy in copies(block, template):
                copy.wait()


def exchange(values, axis, pairs_of):
    size = lax.axis_size(axis)
    return lax.ppermute(values, axis, [(i, pairs_of(i)) for i in range(size)])


def near(value):
    return pltpu.with_memory_space_constraint(value, pltpu.VMEM)


def body(strain, lengths, templates):
    blocks_here, local = strain.shape
    count, order = templates.shape[1], templates.shape[-1]
    half = order // 2
    rows = half + 16
    banks, groups = lax.axis_size("bank"), lax.axis_size("tm")
    bank = lax.axis_index("bank")
    table = tables(order)
    vmem = pl.BlockSpec(memory_space=pltpu.VMEM)
    limit = pltpu.CompilerParams(vmem_limit_bytes=20 * 1024 * 1024)

    index = bank * local + jnp.arange(local, dtype=jnp.int32)
    valid = index[None, :] < lengths[:, None]
    gated = jnp.where(valid, strain, 0.0).astype(bf16).reshape(blocks_here, local // order, order)
    pieces = [gated] + [exchange(gated, "bank", lambda i, s=s: i ^ s) for s in range(1, banks)]

    folded, factor = pl.pallas_call(
        template_kernel,
        grid=(count,),
        in_specs=[pl.BlockSpec((2, 1, order, order), lambda t: (0, t, 0, 0))],
        out_specs=[
            pl.BlockSpec((1, 2, rows, order), lambda t: (t, 0, 0, 0)),
            pl.BlockSpec((1, 8, 128), lambda t: (t, 0, 0)),
        ],
        out_shape=[
            jax.ShapeDtypeStruct((count, 2, rows, order), bf16),
            jax.ShapeDtypeStruct((count, 8, 128), f32),
        ],
        cost_estimate=pl.CostEstimate(flops=int(6e9), bytes_accessed=int(6.5e6), transcendentals=0),
        compiler_params=limit,
        name="fold_templates",
    )(templates)
    *pieces, factor = lax.optimization_barrier((*pieces, factor))

    plane = pltpu.VMEM((2, rows, order), bf16)
    square = pltpu.VMEM((order, order), bf16)
    chunk = rows * order // 128 // (2 * banks)
    kept, later, mine, other, last_block = pl.pallas_call(
        functools.partial(spectrum_kernel, shards=banks),
        in_specs=[vmem] * (banks + 3),
        out_specs=[vmem] * 5,
        out_shape=[plane, plane]
        + [pltpu.VMEM((chunk, 128), bf16)] * 2
        + [pltpu.VMEM((half, order), bf16)],
        scratch_shapes=[
            pltpu.VMEM((blocks_here, half, order), bf16),
            pltpu.VMEM((rows * order // 128, 128), f32),
            square,
            square,
        ],
        cost_estimate=pl.CostEstimate(flops=int(2e9), bytes_accessed=int(5e6), transcendentals=0),
        compiler_params=limit,
        name="spectra",
    )(*map(near, pieces), table["first"], table["twist"], table["sections"])

    partner = exchange(other, "tm", lambda i: i ^ 1)
    chip = (mine.astype(f32) + partner.astype(f32)).astype(bf16)
    share = chip.astype(f32)
    for step in range(1, groups // 2):
        share = share + exchange(chip, "tm", lambda i, s=step: i ^ (2 * s)).astype(f32)
    share = share.astype(bf16)

    before = lax.ppermute(last_block, "tm", [(i, i + 1) for i in range(groups - 1)])
    earlier = pl.pallas_call(
        previous_kernel,
        in_specs=[vmem] * 5,
        out_specs=vmem,
        out_shape=plane,
        scratch_shapes=[square, square],
        cost_estimate=pl.CostEstimate(flops=int(1e9), bytes_accessed=int(4e6), transcendentals=0),
        compiler_params=limit,
        name="previous",
    )(near(before), near(kept), table["first"], table["twist"], table["sections"])

    shares = [share] + [exchange(share, "bank", lambda i, s=s: i ^ s) for s in range(1, banks)]
    *shares, earlier = lax.optimization_barrier((*shares, earlier))
    mine = jnp.stack(shares)
    theirs = exchange(mine, "tm", lambda i: i ^ 1)

    lanes = order // 128
    pairs = blocks_here * count
    out = pl.pallas_call(
        functools.partial(filter_kernel, blocks=float(blocks_here * groups)),
        in_specs=[vmem] * 9,
        out_specs=pl.BlockSpec(memory_space=pl.ANY),
        out_shape=jax.ShapeDtypeStruct((blocks_here * half, lanes * count, 1, 128), f32),
        scratch_shapes=[
            pltpu.VMEM((rows * lanes, 128), f32),
            pltpu.VMEM((blocks_here, 2, rows, order), bf16),
            square,
            square,
            pltpu.VMEM((pairs, order, order), bf16),
            pltpu.VMEM((pairs, half, order), f32),
            pltpu.SemaphoreType.DMA((pairs,)),
        ],
        cost_estimate=pl.CostEstimate(flops=int(6e9), bytes_accessed=int(1.2e7), transcendentals=0),
        compiler_params=limit,
        name="filter",
    )(
        near(mine), near(theirs), near(earlier), near(later), near(folded), near(factor),
        table["twist"], table["sections"], table["last"],
    )
    split = out.reshape(blocks_here * half * lanes, count, 128)
    return jnp.swapaxes(split, 0, 1).reshape(count, blocks_here * half * order)


def solution(mesh):
    in_specs = (P("tm", "bank"), P("tm"), P(None, "bank", None, None))
    out_specs = P("bank", "tm")
    return jax.shard_map(body, mesh=mesh, in_specs=in_specs, out_specs=out_specs, check_vma=False)
```

```python
import functools
import math

import jax
import jax.numpy as jnp
import numpy as np
from jax import lax
from jax.experimental import pallas as pl
from jax.experimental.pallas import tpu as pltpu
from jax.sharding import PartitionSpec as P

epsilon = 1e-06
bf16 = jnp.bfloat16
f32 = jnp.float32
group_order = (0, 2, 1, 3)


def dot(a, b):
    return jnp.dot(a, b, preferred_element_type=f32)


def tables(order):
    half, group = order // 2, order // 4
    rows = half + 16
    a = np.concatenate([np.arange(group), half - np.arange(group), [group], np.zeros(15, np.int64)])
    keep = (np.arange(rows) <= half)[:, None]
    turn = 2.0 * math.pi / order

    def angle(left, right):
        return turn * ((left[:, None] * right[None, :]) % order)

    u, v, g = np.arange(half), np.arange(order), np.arange(group)
    first = np.concatenate([np.cos(angle(a, u)) * keep, -np.sin(angle(a, u)) * keep])
    twist = (2.0 * math.pi / order**2) * (a[:, None] * v[None, :])
    forward, inverse = [], []
    for q in range(4):
        c, s = np.cos(angle(g, 4 * g + q)), np.sin(angle(g, 4 * g + q))
        forward.append(np.block([[c, -s], [s, c]]))
        inverse.append(np.block([[c.T, s.T], [-s.T, c.T]]))
    last = []
    for parity in range(2):
        w = 2 * g + parity
        c, s = np.cos(angle(w, g)), -np.sin(angle(w, g))
        c[:, 0] = 0.5
        s[:, 0] = (1.0 - 2.0 * parity) * (1.0 - 2.0 * (g % 2))
        last.append(np.concatenate([c, s], axis=1))
    return dict(
        first=first.astype(bf16),
        twist=np.stack([np.cos(twist), np.sin(twist)]).astype(np.float32),
        forward=np.stack(forward).astype(bf16),
        inverse=np.stack(inverse).astype(bf16),
        last=np.stack(last).astype(bf16),
    )


def quarters(value):
    group = value.shape[1] // 4
    return [value[:, q * group : (q + 1) * group] for q in range(4)]


def spectrum(samples, first, twist, forward):
    rows = first.shape[0] // 2
    out = dot(first[...], samples)
    real, imag = out[:rows], out[rows:]
    tc, ts = twist[0], twist[1]
    r = quarters(real * tc + imag * ts)
    i = quarters(imag * tc - real * ts)
    ar, ai, br, bi = r[0] + r[2], i[0] + i[2], r[1] + r[3], i[1] + i[3]
    cr, ci, dr, di = r[0] - r[2], i[0] - i[2], r[1] - r[3], i[1] - i[3]
    parts = [(ar + br, ai + bi), (cr + di, ci - dr), (ar - br, ai - bi), (cr - di, ci + dr)]
    return [
        dot(jnp.concatenate(part, axis=1).astype(bf16), forward[q]) for q, part in enumerate(parts)
    ]


def alternate(values):
    row = lax.broadcasted_iota(jnp.int32, values.shape, 0)
    return jnp.where(row % 2 == 0, values, -values)


def spectrum_kernel(*refs, shards):
    pieces = refs[:shards]
    first, twist, forward = refs[shards : shards + 3]
    kept, summed, mine, other, last_block, samples, power = refs[shards + 3 :]
    rows = first.shape[0] // 2
    group = forward.shape[1] // 2
    piece_rows = pieces[0].shape[1]
    bank, core = lax.axis_index("bank"), lax.rem(lax.axis_index("tm"), 2)
    for s in range(shards):
        at = pl.multiple_of((bank ^ s) * piece_rows, piece_rows)
        samples[:, pl.ds(at, piece_rows), :] = pieces[s][...]
    last_block[...] = samples[1]
    ones = spectrum(samples[0], first, twist, forward)
    twos = spectrum(samples[1], first, twist, forward)
    for place, q in enumerate(group_order):
        one, two = ones[q], twos[q]
        cols = slice(place * group, (place + 1) * group)
        for part in range(2):
            x0 = one[:, part * group : (part + 1) * group]
            x1 = two[:, part * group : (part + 1) * group]
            kept[part, :, cols] = x0.astype(bf16)
            summed[part, :, cols] = (x1 + alternate(x0)).astype(bf16)
        total = one * one + two * two
        total = total[:, :group] + total[:, group:]
        lanes = group // 128
        for lane in range(lanes):
            row = (place * lanes + lane) * rows
            power[row : row + rows, :] = total[:, lane * 128 : (lane + 1) * 128]
    chunk = mine.shape[0]
    for dest, which in ((mine, core), (other, 1 - core)):
        at = pl.multiple_of((bank * 2 + which) * chunk, 8)
        dest[...] = power[pl.ds(at, chunk), :].astype(bf16)


def previous_kernel(samples, kept, first, twist, forward, summed):
    group = forward.shape[1] // 2
    parts = spectrum(samples[...], first, twist, forward)
    for place, q in enumerate(group_order):
        x = parts[q]
        cols = slice(place * group, (place + 1) * group)
        for part in range(2):
            added = alternate(x[:, part * group : (part + 1) * group])
            summed[part, :, cols] = (kept[part, :, cols].astype(f32) + added).astype(bf16)


def template_kernel(templates, folded, factor, select):
    order = templates.shape[-1]
    half, group = order // 2, order // 4

    @pl.when(pl.program_id(0) == 0)
    def _():
        m = lax.broadcasted_iota(jnp.int32, (order, order), 0)
        n = lax.broadcasted_iota(jnp.int32, (order, order), 1)
        place = n // group
        source = 4 * (n % group) + jnp.where((place == 1) | (place == 2), 3 - place, place)
        select[:order] = jnp.where(m == source, 1.0, 0.0).astype(bf16)
        select[order:] = jnp.where(m == order - 1 - source, 1.0, 0.0).astype(bf16)

    i = lax.broadcasted_iota(jnp.int32, (group, group), 0)
    r = lax.broadcasted_iota(jnp.int32, (group, group), 1)
    flip = jnp.where(r == group - i, 1.0, 0.0).astype(bf16)
    start = lax.broadcasted_iota(jnp.int32, (group, order), 0) == 0
    energy = jnp.zeros((8, order), f32)
    for part in range(2):
        whole = templates[part, 0]
        wide = whole.astype(f32)
        energy = energy + jnp.sum((wide * wide).reshape(order // 8, 8, order), axis=0)

        def flipped(at, head):
            return jnp.where(start, head, dot(flip, whole[at : at + group])).astype(bf16)

        turned = pltpu.roll(wide[:8], order - 1, 1)[:1]
        upper = [whole[:group], flipped(group, wide[half : half + 1]), whole[group : group + 16]]
        lower = [flipped(half + group, turned), whole[half : half + group], whole[half + group : half + group + 16]]
        lower = jnp.concatenate(lower)
        if part == 1:
            lower = -lower
        both = jnp.concatenate([jnp.concatenate(upper), lower], axis=1)
        for k in range(0, order, half):
            folded[0, part, :, k : k + half] = dot(both, select[:, k : k + half]).astype(bf16)
    total = jnp.sum(jnp.sum(energy, axis=1, keepdims=True), axis=0, keepdims=True)
    factor[0] = jnp.broadcast_to(lax.rsqrt(total), factor.shape[1:])


def filter_scratch(blocks, count, rows, order):
    half, pairs = order // 2, blocks * count
    return [
        pltpu.VMEM((rows * order // 128, 128), f32),
        pltpu.VMEM((blocks, 2, rows, order), bf16),
        pltpu.VMEM((2, rows, order), bf16),
        pltpu.VMEM((2, 4, rows, half), bf16),
        pltpu.VMEM((2, 2, 2, half, half), bf16),
        pltpu.VMEM((pairs, 2, half // 2, order), f32),
        pltpu.SemaphoreType.DMA((pairs,)),
    ]


def filter_kernel(
    mine, theirs, earlier, later, folded, factor, twist, inverse, last, out,
    weight, white, turn, sums, back, result, sems, *, blocks
):
    group = last.shape[1]
    half, order = 2 * group, 4 * group
    rows = twist.shape[1]
    count = folded.shape[0]
    lanes = order // 128
    chunk = mine.shape[1]
    bank, own = lax.axis_index("bank"), lax.rem(lax.axis_index("tm"), 2)
    for s in range(mine.shape[0]):
        for pieces, core in ((mine, own), (theirs, 1 - own)):
            at = pl.multiple_of(((bank ^ s) * 2 + core) * chunk, 8)
            total = pieces[s].astype(f32)
            weight[pl.ds(at, chunk), :] = lax.rsqrt(total / blocks + epsilon)
    turn[...] = twist[...].astype(bf16)

    def copies(slot):
        block, template = divmod(slot, count)
        return [
            pltpu.make_async_copy(
                result.at[slot, parity, :, pl.ds(lane * 128, 128)],
                out.at[pl.ds(block * group, group), parity, lane * count + template, 0, :],
                sems.at[slot],
            )
            for parity in range(2)
            for lane in range(lanes)
        ]

    def whiten(block, side):
        spectra = (earlier, later)[block]
        cols = slice(side * half, (side + 1) * half)
        tiles = range(side * half // 128, (side + 1) * half // 128)
        scale = jnp.concatenate([weight[t * rows : (t + 1) * rows, :] for t in tiles], axis=1)
        for part in range(2):
            white[block, part, :, cols] = (spectra[part, :, cols].astype(f32) * scale).astype(bf16)

    def products(slot, side):
        block, template = divmod(slot, count)
        if template == 0:
            whiten(block, side)
        cols = slice(side * half, (side + 1) * half)
        vr, vi = white[block, 0, :, cols], white[block, 1, :, cols]
        gr, gi = folded[template, 0, :, cols], folded[template, 1, :, cols]
        pr = gr * vr + gi * vi
        pi = gr * vi - gi * vr
        one, two = (
            dot(jnp.concatenate([pr[:, here], pi[:, here]], axis=1), inverse[group_order[2 * side + k]])
            for k, here in enumerate((slice(0, group), slice(group, half)))
        )
        plus, minus = one + two, one - two
        if side == 0:
            real, imag = (plus[:, :group], minus[:, :group]), (plus[:, group:], minus[:, group:])
        else:
            real, imag = (plus[:, :group], two[:, group:] - one[:, group:]), (plus[:, group:], minus[:, :group])
        sums[slot % 2, 2 * side] = jnp.concatenate(real, axis=1).astype(bf16)
        sums[slot % 2, 2 * side + 1] = jnp.concatenate(imag, axis=1).astype(bf16)

    def turned(slot, at, size):
        here = slice(at, at + size)
        r0, i0, r1, i1 = (sums[slot % 2, plane, here] for plane in range(4))
        values = []
        for side, (ir, ii) in enumerate(((r0 + r1, i0 + i1), (r0 - r1, i0 - i1))):
            cols = slice(side * half, (side + 1) * half)
            tc, ts = turn[0, here, cols], turn[1, here, cols]
            values.append((ir * tc - ii * ts, ii * tc + ir * ts))
        return values

    def twists(slot, part, parts):
        step = 16
        first = lax.broadcasted_iota(jnp.int32, (step, half), 0) == 0
        span = group // parts
        for at in range(part * span, (part + 1) * span, step):
            near_rows, far_rows = turned(slot, at, step), turned(slot, group + at, step)
            middle = turned(slot, half, step) if at == 0 else None
            for side in range(2):
                (r0, i0), (r1, i1) = near_rows[side], far_rows[side]
                for parity in range(2):
                    re, im = (r0 + r1, i0 - i1) if parity == 0 else (r0 - r1, i0 + i1)
                    if at == 0:
                        row = middle[side][parity][:1].astype(f32)
                        im = jnp.where(first, jnp.broadcast_to(row, im.shape), im.astype(f32)).astype(bf16)
                    back[slot % 2, parity, side, at : at + step] = re
                    back[slot % 2, parity, side, group + at : group + at + step] = im

    def finish(slot, parity, side):
        scale = factor[slot % count, 0:1, 0:1]
        value = dot(last[parity], back[slot % 2, parity, side])
        result[slot, parity, :, side * half : (side + 1) * half] = value * scale

    total = 2 * count
    for step in range(total + 2):
        for j in range(2):
            if step < total:
                products(step, j)
            if 0 <= step - 2:
                finish(step - 2, j, 0)
                finish(step - 2, j, 1)
            if 0 <= step - 1 < total:
                twists(step - 1, j, 2)
        if 0 <= step - 2:
            for copy in copies(step - 2):
                copy.start()
    for slot in range(total):
        for copy in copies(slot):
            copy.wait()


def exchange(values, axis, pairs_of):
    size = lax.axis_size(axis)
    return lax.ppermute(values, axis, [(i, pairs_of(i)) for i in range(size)])


def near(value):
    return pltpu.with_memory_space_constraint(value, pltpu.VMEM)


def body(strain, lengths, templates):
    blocks_here, local = strain.shape
    count, order = templates.shape[1], templates.shape[-1]
    half = order // 2
    rows = half + 16
    banks, groups = lax.axis_size("bank"), lax.axis_size("tm")
    bank = lax.axis_index("bank")
    table = tables(order)
    vmem = pl.BlockSpec(memory_space=pltpu.VMEM)
    limit = pltpu.CompilerParams(vmem_limit_bytes=20 * 1024 * 1024)

    index = bank * local + jnp.arange(local, dtype=jnp.int32)
    valid = index[None, :] < lengths[:, None]
    gated = jnp.where(valid, strain, 0.0).astype(bf16).reshape(blocks_here, local // order, order)
    pieces = [gated] + [exchange(gated, "bank", lambda i, s=s: i ^ s) for s in range(1, banks)]

    folded, factor = pl.pallas_call(
        template_kernel,
        grid=(count,),
        in_specs=[pl.BlockSpec((2, 1, order, order), lambda t: (0, t, 0, 0))],
        out_specs=[
            pl.BlockSpec((1, 2, rows, order), lambda t: (t, 0, 0, 0)),
            pl.BlockSpec((1, 8, 128), lambda t: (t, 0, 0)),
        ],
        out_shape=[
            jax.ShapeDtypeStruct((count, 2, rows, order), bf16),
            jax.ShapeDtypeStruct((count, 8, 128), f32),
        ],
        scratch_shapes=[pltpu.VMEM((2 * order, order), bf16)],
        cost_estimate=pl.CostEstimate(flops=int(6e9), bytes_accessed=int(6.5e6), transcendentals=0),
        compiler_params=limit,
        name="fold_templates",
    )(pltpu.with_memory_space_constraint(templates, pltpu.HBM))
    *pieces, factor = lax.optimization_barrier((*pieces, factor))

    plane = pltpu.VMEM((2, rows, order), bf16)
    chunk = rows * order // 128 // (2 * banks)
    kept, later, mine, other, last_block = pl.pallas_call(
        functools.partial(spectrum_kernel, shards=banks),
        in_specs=[vmem] * (banks + 3),
        out_specs=[vmem] * 5,
        out_shape=[plane, plane]
        + [pltpu.VMEM((chunk, 128), bf16)] * 2
        + [pltpu.VMEM((half, order), bf16)],
        scratch_shapes=[
            pltpu.VMEM((blocks_here, half, order), bf16),
            pltpu.VMEM((rows * order // 128, 128), f32),
        ],
        cost_estimate=pl.CostEstimate(flops=int(2e9), bytes_accessed=int(5e6), transcendentals=0),
        compiler_params=limit,
        name="spectra",
    )(*map(near, pieces), table["first"], table["twist"], table["forward"])

    partner = exchange(other, "tm", lambda i: i ^ 1)
    chip = (mine.astype(f32) + partner.astype(f32)).astype(bf16)
    share = chip.astype(f32)
    for step in range(1, groups // 2):
        share = share + exchange(chip, "tm", lambda i, s=step: i ^ (2 * s)).astype(f32)
    share = share.astype(bf16)

    before = lax.ppermute(last_block, "tm", [(i, i + 1) for i in range(groups - 1)])
    earlier = pl.pallas_call(
        previous_kernel,
        in_specs=[vmem] * 5,
        out_specs=vmem,
        out_shape=plane,
        cost_estimate=pl.CostEstimate(flops=int(1e9), bytes_accessed=int(4e6), transcendentals=0),
        compiler_params=limit,
        name="previous",
    )(near(before), near(kept), table["first"], table["twist"], table["forward"])

    shares = [share] + [exchange(share, "bank", lambda i, s=s: i ^ s) for s in range(1, banks)]
    *shares, earlier = lax.optimization_barrier((*shares, earlier))
    mine = jnp.stack(shares)
    theirs = exchange(mine, "tm", lambda i: i ^ 1)

    lanes = order // 128
    out = pl.pallas_call(
        functools.partial(filter_kernel, blocks=float(blocks_here * groups)),
        in_specs=[vmem] * 9,
        out_specs=pl.BlockSpec(memory_space=pl.ANY),
        out_shape=jax.ShapeDtypeStruct((blocks_here * half // 2, 2, lanes * count, 1, 128), f32),
        scratch_shapes=filter_scratch(blocks_here, count, rows, order),
        cost_estimate=pl.CostEstimate(flops=int(6e9), bytes_accessed=int(1.2e7), transcendentals=0),
        compiler_params=limit,
        name="filter",
    )(
        near(mine), near(theirs), near(earlier), near(later), near(folded), near(factor),
        table["twist"], table["inverse"], table["last"],
    )
    split = out.reshape(blocks_here * half * lanes, count, 128)
    return jnp.swapaxes(split, 0, 1).reshape(count, blocks_here * half * order)


def solution(mesh):
    in_specs = (P("tm", "bank"), P("tm"), P(None, "bank", None, None))
    out_specs = P("bank", "tm")
    return jax.shard_map(body, mesh=mesh, in_specs=in_specs, out_specs=out_specs, check_vma=False)
```

```python
import functools
import math

import jax
import jax.numpy as jnp
import numpy as np
from jax import lax
from jax.experimental import pallas as pl
from jax.experimental.pallas import tpu as pltpu
from jax.sharding import PartitionSpec as P

epsilon = 1e-06
bf16 = jnp.bfloat16
f32 = jnp.float32
group_order = (0, 2, 1, 3)


def dot(a, b):
    return jnp.dot(a, b, preferred_element_type=f32)


def tables(order):
    half, group, eighth = order // 2, order // 4, order // 8
    i, pad = np.arange(group), np.zeros(8, np.int64)
    middle = np.concatenate([[group], pad[1:]])
    a = np.concatenate([i[:eighth], half - i[:eighth], middle, i[eighth:], half - i[eighth:], pad])
    rows = half + 16
    keep = np.ones((rows, 1))
    keep[group + 1 : group + 8] = 0
    keep[rows - 8 :] = 0
    turn = 2.0 * math.pi / order

    def angle(left, right):
        return turn * ((left[:, None] * right[None, :]) % order)

    u, v, g = np.arange(half), np.arange(order), np.arange(group)
    first = np.concatenate([np.cos(angle(a, u)) * keep, -np.sin(angle(a, u)) * keep])
    twist = (2.0 * math.pi / order**2) * (a[:, None] * v[None, :])
    forward, inverse = [], []
    for q in range(4):
        c, s = np.cos(angle(g, 4 * g + q)), np.sin(angle(g, 4 * g + q))
        forward.append(np.block([[c, -s], [s, c]]))
        inverse.append(np.block([[c.T, s.T], [-s.T, c.T]]))
    last = []
    for parity in range(2):
        w = 2 * g + parity
        c, s = np.cos(angle(w, g)), -np.sin(angle(w, g))
        c[:, 0] = 0.5
        s[:, 0] = (1.0 - 2.0 * parity) * (1.0 - 2.0 * (g % 2))
        sides = [np.concatenate([c[:, h], s[:, h]], axis=1) for h in (slice(0, eighth), slice(eighth, group))]
        last.append([np.concatenate([sides[core], sides[1 - core]], axis=1) for core in range(2)])
    return dict(
        first=first.astype(bf16),
        twist=np.stack([np.cos(twist), np.sin(twist)]).astype(np.float32),
        forward=np.stack(forward).astype(bf16),
        inverse=np.stack(inverse).astype(bf16),
        last=np.stack(last).astype(bf16),
    )


def quarters(value):
    group = value.shape[1] // 4
    return [value[:, q * group : (q + 1) * group] for q in range(4)]


def spectrum(samples, first, twist, forward):
    rows = first.shape[0] // 2
    out = dot(first[...], samples)
    real, imag = out[:rows], out[rows:]
    tc, ts = twist[0], twist[1]
    r = quarters(real * tc + imag * ts)
    i = quarters(imag * tc - real * ts)
    ar, ai, br, bi = r[0] + r[2], i[0] + i[2], r[1] + r[3], i[1] + i[3]
    cr, ci, dr, di = r[0] - r[2], i[0] - i[2], r[1] - r[3], i[1] - i[3]
    parts = [(ar + br, ai + bi), (cr + di, ci - dr), (ar - br, ai - bi), (cr - di, ci + dr)]
    return [
        dot(jnp.concatenate(part, axis=1).astype(bf16), forward[q]) for q, part in enumerate(parts)
    ]


def alternate(values):
    row = lax.broadcasted_iota(jnp.int32, values.shape, 0)
    return jnp.where(row % 2 == 0, values, -values)


def spectrum_kernel(*refs, shards):
    pieces = refs[:shards]
    first, twist, forward = refs[shards : shards + 3]
    kept, summed, mine, other, last_block, samples, power = refs[shards + 3 :]
    rows = first.shape[0] // 2
    group = forward.shape[1] // 2
    piece_rows = pieces[0].shape[1]
    bank, core = lax.axis_index("bank"), lax.rem(lax.axis_index("tm"), 2)
    for s in range(shards):
        at = pl.multiple_of((bank ^ s) * piece_rows, piece_rows)
        samples[:, pl.ds(at, piece_rows), :] = pieces[s][...]
    last_block[...] = samples[1]
    ones = spectrum(samples[0], first, twist, forward)
    twos = spectrum(samples[1], first, twist, forward)
    for place, q in enumerate(group_order):
        one, two = ones[q], twos[q]
        cols = slice(place * group, (place + 1) * group)
        for part in range(2):
            x0 = one[:, part * group : (part + 1) * group]
            x1 = two[:, part * group : (part + 1) * group]
            kept[part, :, cols] = x0.astype(bf16)
            summed[part, :, cols] = (x1 + alternate(x0)).astype(bf16)
        total = one * one + two * two
        total = total[:, :group] + total[:, group:]
        lanes = group // 128
        for lane in range(lanes):
            row = (place * lanes + lane) * rows
            power[row : row + rows, :] = total[:, lane * 128 : (lane + 1) * 128]
    chunk = mine.shape[0]
    for dest, which in ((mine, core), (other, 1 - core)):
        at = pl.multiple_of((bank * 2 + which) * chunk, 8)
        dest[...] = power[pl.ds(at, chunk), :].astype(bf16)


def previous_kernel(samples, kept, first, twist, forward, summed):
    group = forward.shape[1] // 2
    follows = lax.axis_index("tm") > 0
    parts = spectrum(jnp.where(follows, samples[...].astype(f32), 0.0).astype(bf16), first, twist, forward)
    for place, q in enumerate(group_order):
        x = parts[q]
        cols = slice(place * group, (place + 1) * group)
        for part in range(2):
            added = alternate(x[:, part * group : (part + 1) * group])
            summed[part, :, cols] = (kept[part, :, cols].astype(f32) + added).astype(bf16)


def template_kernel(templates, folded, factor, select):
    order = templates.shape[-1]
    half, group = order // 2, order // 4

    @pl.when(pl.program_id(0) == 0)
    def _():
        m = lax.broadcasted_iota(jnp.int32, (order, order), 0)
        n = lax.broadcasted_iota(jnp.int32, (order, order), 1)
        place = n // group
        source = 4 * (n % group) + jnp.where((place == 1) | (place == 2), 3 - place, place)
        select[:order] = jnp.where(m == source, 1.0, 0.0).astype(bf16)
        select[order:] = jnp.where(m == order - 1 - source, 1.0, 0.0).astype(bf16)

    i = lax.broadcasted_iota(jnp.int32, (group, group), 0)
    r = lax.broadcasted_iota(jnp.int32, (group, group), 1)
    flip = jnp.where(r == group - i, 1.0, 0.0).astype(bf16)
    start = lax.broadcasted_iota(jnp.int32, (group, order), 0) == 0
    energy = jnp.zeros((8, order), f32)
    for part in range(2):
        whole = templates[part, 0]
        wide = whole.astype(f32)
        energy = energy + jnp.sum((wide * wide).reshape(order // 8, 8, order), axis=0)

        def flipped(at, head):
            return jnp.where(start, head, dot(flip, whole[at : at + group])).astype(bf16)

        turned = pltpu.roll(wide[:8], order - 1, 1)[:1]
        mirror, wrapped = flipped(group, wide[half : half + 1]), flipped(half + group, turned)
        upper, lower = [], []
        for h in range(2):
            near_rows = slice(h * (group // 2), (h + 1) * (group // 2))
            upper += [whole[near_rows], mirror[near_rows], whole[group + 8 * h : group + 8 * h + 8]]
            at = half + h * (group // 2)
            lower += [wrapped[near_rows], whole[at : at + group // 2]]
            lower += [whole[half + group + 8 * h : half + group + 8 * h + 8]]
        lower = jnp.concatenate(lower)
        if part == 1:
            lower = -lower
        both = jnp.concatenate([jnp.concatenate(upper), lower], axis=1)
        for k in range(0, order, half):
            folded[0, part, :, k : k + half] = dot(both, select[:, k : k + half]).astype(bf16)
    total = jnp.sum(jnp.sum(energy, axis=1, keepdims=True), axis=0, keepdims=True)
    factor[0] = jnp.broadcast_to(lax.rsqrt(total), factor.shape[1:])


def section_rows(folded, white, inverse, block, template, side, here, put):
    group = inverse.shape[1] // 2
    half = 2 * group
    cols = slice(side * half, (side + 1) * half)
    vr, vi = white[block, 0, :, cols], white[block, 1, :, cols]
    gr, gi = folded[template, 0, here, cols], folded[template, 1, here, cols]
    pr = gr * vr + gi * vi
    pi = gr * vi - gi * vr
    one, two = (
        dot(jnp.concatenate([pr[:, part], pi[:, part]], axis=1), inverse[group_order[2 * side + k]])
        for k, part in enumerate((slice(0, group), slice(group, half)))
    )
    plus, minus = one + two, one - two
    if side == 0:
        real, imag = (plus[:, :group], minus[:, :group]), (plus[:, group:], minus[:, group:])
    else:
        real, imag = (plus[:, :group], two[:, group:] - one[:, group:]), (plus[:, group:], minus[:, :group])
    put(2 * side, jnp.concatenate(real, axis=1).astype(bf16))
    put(2 * side + 1, jnp.concatenate(imag, axis=1).astype(bf16))


def fill_weights(pieces, weight, blocks):
    bank = lax.axis_index("bank")
    chunk = pieces.shape[1]
    for s in range(pieces.shape[0]):
        at = pl.multiple_of((bank ^ s) * chunk, 8)
        weight[pl.ds(at, chunk), :] = lax.rsqrt(pieces[s].astype(f32) / blocks + epsilon)


def whiten_rows(spectra, weight, white, block, side, here):
    chunk, half = white.shape[2], white.shape[3] // 2
    cols = slice(side * half, (side + 1) * half)
    tiles = range(side * half // 128, (side + 1) * half // 128)
    scale = jnp.concatenate([weight[t * chunk : (t + 1) * chunk, :] for t in tiles], axis=1)
    for part in range(2):
        white[block, part, :, cols] = (spectra[part, here, cols].astype(f32) * scale).astype(bf16)


def turned(sums, turn, at, size):
    span = slice(at, at + size)
    half = sums.shape[2]
    r0, i0, r1, i1 = (sums[plane, span] for plane in range(4))
    values = []
    for side, (ir, ii) in enumerate(((r0 + r1, i0 + i1), (r0 - r1, i0 - i1))):
        cols = slice(side * half, (side + 1) * half)
        tc, ts = turn[0, span, cols], turn[1, span, cols]
        values.append((ir * tc - ii * ts, ii * tc + ir * ts))
    return values


def twists(sums, turn, which, part, parts, put):
    half = sums.shape[2]
    near_count = half // 4
    step = 16
    first = (lax.broadcasted_iota(jnp.int32, (step, half), 0) == 0) & (which == 0)
    for at in range(part * near_count // parts, (part + 1) * near_count // parts, step):
        near_rows, far_rows = turned(sums, turn, at, step), turned(sums, turn, near_count + at, step)
        middle = turned(sums, turn, 2 * near_count, 8) if at == 0 else None
        for side in range(2):
            (r0, i0), (r1, i1) = near_rows[side], far_rows[side]
            for parity in range(2):
                re, im = (r0 + r1, i0 - i1) if parity == 0 else (r0 - r1, i0 + i1)
                if at == 0:
                    row = middle[side][parity][:1].astype(f32)
                    im = jnp.where(first, jnp.broadcast_to(row, im.shape), im.astype(f32)).astype(bf16)
                put(parity, side, at, re)
                put(parity, side, near_count + at, im)


def own_rows_kernel(
    mine, earlier, later, folded, twist, inverse, back, weight, white, turn, even_sums, odd_sums, *, blocks
):
    chunk, count = white.shape[2], folded.shape[0]
    core = lax.rem(lax.axis_index("tm"), 2)
    here = pl.ds(pl.multiple_of(core * chunk, 8), chunk)
    fill_weights(mine, weight, blocks)
    turn[...] = twist[:, here, :].astype(bf16)
    total = 2 * count
    for slot in range(total + 1):
        for j in range(2):
            if slot < total:
                block, template = divmod(slot, count)
                sums = (even_sums, odd_sums)[slot % 2]
                if template == 0:
                    whiten_rows((earlier, later)[block], weight, white, block, j, here)

                def put_sums(plane, value):
                    sums[plane] = value

                section_rows(folded, white, inverse, block, template, j, here, put_sums)
            if slot > 0:

                def put_back(parity, side, at, value):
                    back[slot - 1, parity, side, at : at + value.shape[0]] = value

                twists((even_sums, odd_sums)[(slot - 1) % 2], turn, core, j, 2, put_back)


def own_scratch(blocks, rows, order):
    half = order // 2
    return [
        pltpu.VMEM((rows // 2 * order // 128, 128), f32),
        pltpu.VMEM((blocks, 2, rows // 2, order), bf16),
        pltpu.VMEM((2, rows // 2, order), bf16),
        pltpu.VMEM((4, rows // 2, half), bf16),
        pltpu.VMEM((4, rows // 2, half), bf16),
    ]


def filter_scratch(blocks, count, rows, order):
    half, pairs = order // 2, blocks * count
    return own_scratch(blocks, rows, order) + [
        pltpu.VMEM((2, 2, half // 2, half), bf16),
        pltpu.VMEM((2, 2, half // 2, half), bf16),
        pltpu.VMEM((pairs, 2, half // 2, order), f32),
        pltpu.SemaphoreType.DMA((pairs,)),
    ]


def filter_kernel(
    theirs, own, earlier, later, folded, factor, twist, inverse, last, out,
    weight, white, turn, even_sums, odd_sums, even_back, odd_back, result, sems, *, blocks
):
    group = last.shape[2]
    half, order = 2 * group, 4 * group
    count, chunk = folded.shape[0], white.shape[2]
    lanes = order // 128
    core = lax.rem(lax.axis_index("tm"), 2)
    there = pl.ds(pl.multiple_of((1 - core) * chunk, 8), chunk)
    fill_weights(theirs, weight, blocks)
    turn[...] = twist[:, there, :].astype(bf16)

    def copies(slot):
        block, template = divmod(slot, count)
        return [
            pltpu.make_async_copy(
                result.at[slot, parity, :, pl.ds(lane * 128, 128)],
                out.at[pl.ds(block * group, group), parity, lane * count + template, 0, :],
                sems.at[slot],
            )
            for parity in range(2)
            for lane in range(lanes)
        ]

    def products(slot, side):
        block, template = divmod(slot, count)
        sums = (even_sums, odd_sums)[slot % 2]
        if template == 0:
            whiten_rows((earlier, later)[block], weight, white, block, side, there)

        def put(plane, value):
            sums[plane] = value

        section_rows(folded, white, inverse, block, template, side, there, put)

    def turns(slot, part):
        back = (even_back, odd_back)[slot % 2]

        def put(parity, side, at, value):
            back[parity, side, at : at + value.shape[0]] = value

        twists((even_sums, odd_sums)[slot % 2], turn, 1 - core, part, 2, put)

    def finish(slot, parity, side):
        back = (even_back, odd_back)[slot % 2]
        scale = factor[slot % count, 0:1, 0:1]
        whole = jnp.concatenate([own[slot, parity, side], back[parity, side]], axis=0)
        result[slot, parity, :, side * half : (side + 1) * half] = dot(last[parity, core], whole) * scale

    total = 2 * count
    for step in range(total + 2):
        for j in range(2):
            if 0 <= step - 1 < total:
                turns(step - 1, j)
            if 0 <= step - 2:
                finish(step - 2, j, 0)
                finish(step - 2, j, 1)
            if step < total:
                products(step, j)
        if step % 2 == 1 and step >= 3:
            for slot in (step - 3, step - 2):
                for copy in copies(slot):
                    copy.start()
    for slot in range(total):
        for copy in copies(slot):
            copy.wait()


def exchange(values, axis, pairs_of):
    size = lax.axis_size(axis)
    return lax.ppermute(values, axis, [(i, pairs_of(i)) for i in range(size)])


def near(value):
    return pltpu.with_memory_space_constraint(value, pltpu.VMEM)


def body(strain, lengths, templates):
    blocks_here, local = strain.shape
    count, order = templates.shape[1], templates.shape[-1]
    half = order // 2
    rows = half + 16
    banks, groups = lax.axis_size("bank"), lax.axis_size("tm")
    bank = lax.axis_index("bank")
    table = tables(order)
    vmem = pl.BlockSpec(memory_space=pltpu.VMEM)
    limit = pltpu.CompilerParams(vmem_limit_bytes=20 * 1024 * 1024)

    index = bank * local + jnp.arange(local, dtype=jnp.int32)
    valid = index[None, :] < lengths[:, None]
    gated = jnp.where(valid, strain, 0.0).astype(bf16).reshape(blocks_here, local // order, order)
    pieces = [gated] + [exchange(gated, "bank", lambda i, s=s: i ^ s) for s in range(1, banks)]

    folded, factor = pl.pallas_call(
        template_kernel,
        grid=(count,),
        in_specs=[pl.BlockSpec((2, 1, order, order), lambda t: (0, t, 0, 0))],
        out_specs=[
            pl.BlockSpec((1, 2, rows, order), lambda t: (t, 0, 0, 0)),
            pl.BlockSpec((1, 8, 128), lambda t: (t, 0, 0)),
        ],
        out_shape=[
            jax.ShapeDtypeStruct((count, 2, rows, order), bf16),
            jax.ShapeDtypeStruct((count, 8, 128), f32),
        ],
        scratch_shapes=[pltpu.VMEM((2 * order, order), bf16)],
        cost_estimate=pl.CostEstimate(flops=int(6e9), bytes_accessed=int(6.5e6), transcendentals=0),
        compiler_params=limit,
        name="fold_templates",
    )(pltpu.with_memory_space_constraint(templates, pltpu.HBM))
    *pieces, factor = lax.optimization_barrier((*pieces, factor))

    plane = pltpu.VMEM((2, rows, order), bf16)
    chunk = rows * order // 128 // (2 * banks)
    kept, later, mine, other, last_block = pl.pallas_call(
        functools.partial(spectrum_kernel, shards=banks),
        in_specs=[vmem] * (banks + 3),
        out_specs=[vmem] * 5,
        out_shape=[plane, plane]
        + [pltpu.VMEM((chunk, 128), bf16)] * 2
        + [pltpu.VMEM((half, order), bf16)],
        scratch_shapes=[
            pltpu.VMEM((blocks_here, half, order), bf16),
            pltpu.VMEM((rows * order // 128, 128), f32),
        ],
        cost_estimate=pl.CostEstimate(flops=int(2e9), bytes_accessed=int(5e6), transcendentals=0),
        compiler_params=limit,
        name="spectra",
    )(*map(near, pieces), table["first"], table["twist"], table["forward"])

    partner = exchange(other, "tm", lambda i: i ^ 1)
    chip = (mine.astype(f32) + partner.astype(f32)).astype(bf16)
    share = chip.astype(f32)
    for step in range(1, groups // 2):
        share = share + exchange(chip, "tm", lambda i, s=step: i ^ (2 * s)).astype(f32)
    share = share.astype(bf16)

    before = lax.ppermute(last_block, "tm", [(i, (i + 1) % groups) for i in range(groups)])
    earlier = pl.pallas_call(
        previous_kernel,
        in_specs=[vmem] * 5,
        out_specs=vmem,
        out_shape=plane,
        cost_estimate=pl.CostEstimate(flops=int(1e9), bytes_accessed=int(4e6), transcendentals=0),
        compiler_params=limit,
        name="previous",
    )(near(before), near(kept), table["first"], table["twist"], table["forward"])

    shares = [share] + [exchange(share, "bank", lambda i, s=s: i ^ s) for s in range(1, banks)]
    *shares, earlier = lax.optimization_barrier((*shares, earlier))
    mine = jnp.stack(shares)
    theirs = exchange(mine, "tm", lambda i: i ^ 1)

    lanes = order // 128
    blocks = float(blocks_here * groups)
    own = pl.pallas_call(
        functools.partial(own_rows_kernel, blocks=blocks),
        in_specs=[vmem] * 6,
        out_specs=vmem,
        out_shape=pltpu.VMEM((blocks_here * count, 2, 2, half // 2, half), bf16),
        scratch_shapes=own_scratch(blocks_here, rows, order),
        cost_estimate=pl.CostEstimate(flops=int(2e9), bytes_accessed=int(6e6), transcendentals=0),
        compiler_params=limit,
        name="own_rows",
    )(near(mine), near(earlier), near(later), near(folded), table["twist"], table["inverse"])
    out = pl.pallas_call(
        functools.partial(filter_kernel, blocks=blocks),
        in_specs=[vmem] * 9,
        out_specs=pl.BlockSpec(memory_space=pl.ANY),
        out_shape=jax.ShapeDtypeStruct((blocks_here * half // 2, 2, lanes * count, 1, 128), f32),
        scratch_shapes=filter_scratch(blocks_here, count, rows, order),
        cost_estimate=pl.CostEstimate(flops=int(6e9), bytes_accessed=int(1.2e7), transcendentals=0),
        compiler_params=limit,
        name="filter",
    )(
        near(theirs), near(own), near(earlier), near(later), near(folded), near(factor),
        table["twist"], table["inverse"], table["last"],
    )
    split = out.reshape(blocks_here * half * lanes, count, 128)
    return jnp.swapaxes(split, 0, 1).reshape(count, blocks_here * half * order)


def solution(mesh):
    in_specs = (P("tm", "bank"), P("tm"), P(None, "bank", None, None))
    out_specs = P("bank", "tm")
    return jax.shard_map(body, mesh=mesh, in_specs=in_specs, out_specs=out_specs, check_vma=False)
```

```python
import functools
import math

import jax
import jax.numpy as jnp
import numpy as np
from jax import lax
from jax.experimental import pallas as pl
from jax.experimental.pallas import tpu as pltpu
from jax.sharding import PartitionSpec as P

epsilon = 1e-06
bf16 = jnp.bfloat16
f32 = jnp.float32
group_order = (0, 2, 1, 3)


def dot(a, b):
    return jnp.dot(a, b, preferred_element_type=f32)


def tables(order):
    half, group, eighth = order // 2, order // 4, order // 8
    i, pad = np.arange(group), np.zeros(8, np.int64)
    middle = np.concatenate([[group], pad[1:]])
    a = np.concatenate([i[:eighth], half - i[:eighth], middle, i[eighth:], half - i[eighth:], pad])
    rows = half + 16
    keep = np.ones((rows, 1))
    keep[group + 1 : group + 8] = 0
    keep[rows - 8 :] = 0
    turn = 2.0 * math.pi / order

    def angle(left, right):
        return turn * ((left[:, None] * right[None, :]) % order)

    u, v, g = np.arange(half), np.arange(order), np.arange(group)
    first = np.concatenate([np.cos(angle(a, u)) * keep, -np.sin(angle(a, u)) * keep])
    twist = (2.0 * math.pi / order**2) * (a[:, None] * v[None, :])
    forward, inverse = [], []
    for q in range(4):
        c, s = np.cos(angle(g, 4 * g + q)), np.sin(angle(g, 4 * g + q))
        forward.append(np.block([[c, -s], [s, c]]))
        inverse.append(np.block([[c.T, s.T], [-s.T, c.T]]))
    last = []
    for parity in range(2):
        w = 2 * g + parity
        c, s = np.cos(angle(w, g)), -np.sin(angle(w, g))
        c[:, 0] = 0.5
        s[:, 0] = (1.0 - 2.0 * parity) * (1.0 - 2.0 * (g % 2))
        sides = [np.concatenate([c[:, h], s[:, h]], axis=1) for h in (slice(0, eighth), slice(eighth, group))]
        last.append([np.concatenate([sides[core], sides[1 - core]], axis=1) for core in range(2)])
    return dict(
        first=first.astype(bf16),
        twist=np.stack([np.cos(twist), np.sin(twist)]).astype(np.float32),
        forward=np.stack(forward).astype(bf16),
        inverse=np.stack(inverse).astype(bf16),
        last=np.stack(last).astype(bf16),
    )


def gate_kernel(lengths, strain, gated):
    blocks, count, order = gated.shape
    lanes = order // 128
    start = lax.axis_index("bank") * (count * order)
    row = lax.broadcasted_iota(jnp.int32, (count, 128), 0)
    column = lax.broadcasted_iota(jnp.int32, (count, 128), 1)
    for block in range(blocks):
        for lane in range(lanes):
            x = strain[pl.ds(lane * blocks + block, count, stride=lanes * blocks), :]
            position = start + row * order + lane * 128 + column
            gated[block, :, lane * 128 : (lane + 1) * 128] = jnp.where(
                position < lengths[block], x, 0.0
            ).astype(bf16)


def quarters(value):
    group = value.shape[1] // 4
    return [value[:, q * group : (q + 1) * group] for q in range(4)]


def spectrum(samples, first, twist, forward):
    rows = first.shape[0] // 2
    out = dot(first[...], samples)
    real, imag = out[:rows], out[rows:]
    tc, ts = twist[0], twist[1]
    r = quarters(real * tc + imag * ts)
    i = quarters(imag * tc - real * ts)
    ar, ai, br, bi = r[0] + r[2], i[0] + i[2], r[1] + r[3], i[1] + i[3]
    cr, ci, dr, di = r[0] - r[2], i[0] - i[2], r[1] - r[3], i[1] - i[3]
    parts = [(ar + br, ai + bi), (cr + di, ci - dr), (ar - br, ai - bi), (cr - di, ci + dr)]
    return [
        dot(jnp.concatenate(part, axis=1).astype(bf16), forward[q]) for q, part in enumerate(parts)
    ]


def alternate(values):
    row = lax.broadcasted_iota(jnp.int32, values.shape, 0)
    return jnp.where(row % 2 == 0, values, -values)


def spectrum_kernel(*refs, shards):
    pieces = refs[:shards]
    first, twist, forward = refs[shards : shards + 3]
    kept, summed, mine, other, last_block, samples, power = refs[shards + 3 :]
    rows = first.shape[0] // 2
    group = forward.shape[1] // 2
    piece_rows = pieces[0].shape[1]
    bank, core = lax.axis_index("bank"), lax.rem(lax.axis_index("tm"), 2)
    for s in range(shards):
        at = pl.multiple_of((bank ^ s) * piece_rows, piece_rows)
        samples[:, pl.ds(at, piece_rows), :] = pieces[s][...]
    last_block[...] = samples[1]
    ones = spectrum(samples[0], first, twist, forward)
    twos = spectrum(samples[1], first, twist, forward)
    for place, q in enumerate(group_order):
        one, two = ones[q], twos[q]
        cols = slice(place * group, (place + 1) * group)
        for part in range(2):
            x0 = one[:, part * group : (part + 1) * group]
            x1 = two[:, part * group : (part + 1) * group]
            kept[part, :, cols] = x0.astype(bf16)
            summed[part, :, cols] = (x1 + alternate(x0)).astype(bf16)
        total = one * one + two * two
        total = total[:, :group] + total[:, group:]
        lanes = group // 128
        for lane in range(lanes):
            for h in range(2):
                row = (h * 4 * lanes + place * lanes + lane) * (rows // 2)
                piece = total[h * (rows // 2) : (h + 1) * (rows // 2), lane * 128 : (lane + 1) * 128]
                power[row : row + rows // 2, :] = piece
    chunk = mine.shape[0]
    for dest, which in ((mine, core), (other, 1 - core)):
        at = pl.multiple_of(which * (power.shape[0] // 2) + bank * chunk, 8)
        dest[...] = power[pl.ds(at, chunk), :].astype(bf16)


def previous_kernel(samples, kept, first, twist, forward, summed):
    group = forward.shape[1] // 2
    follows = lax.axis_index("tm") > 0
    parts = spectrum(jnp.where(follows, samples[...].astype(f32), 0.0).astype(bf16), first, twist, forward)
    for place, q in enumerate(group_order):
        x = parts[q]
        cols = slice(place * group, (place + 1) * group)
        for part in range(2):
            added = alternate(x[:, part * group : (part + 1) * group])
            summed[part, :, cols] = (kept[part, :, cols].astype(f32) + added).astype(bf16)


def template_kernel(templates, folded, factor, select):
    order = templates.shape[-1]
    half, group = order // 2, order // 4

    @pl.when(pl.program_id(0) == 0)
    def _():
        m = lax.broadcasted_iota(jnp.int32, (order, order), 0)
        n = lax.broadcasted_iota(jnp.int32, (order, order), 1)
        place = n // group
        source = 4 * (n % group) + jnp.where((place == 1) | (place == 2), 3 - place, place)
        select[:order] = jnp.where(m == source, 1.0, 0.0).astype(bf16)
        select[order:] = jnp.where(m == order - 1 - source, 1.0, 0.0).astype(bf16)

    i = lax.broadcasted_iota(jnp.int32, (group, group), 0)
    r = lax.broadcasted_iota(jnp.int32, (group, group), 1)
    flip = jnp.where(r == group - i, 1.0, 0.0).astype(bf16)
    start = lax.broadcasted_iota(jnp.int32, (group, order), 0) == 0
    energy = jnp.zeros((8, order), f32)
    for part in range(2):
        whole = templates[part, 0]
        wide = whole.astype(f32)
        energy = energy + jnp.sum((wide * wide).reshape(order // 8, 8, order), axis=0)

        def flipped(at, head):
            return jnp.where(start, head, dot(flip, whole[at : at + group])).astype(bf16)

        turned = pltpu.roll(wide[:8], order - 1, 1)[:1]
        mirror, wrapped = flipped(group, wide[half : half + 1]), flipped(half + group, turned)
        upper, lower = [], []
        for h in range(2):
            near_rows = slice(h * (group // 2), (h + 1) * (group // 2))
            upper += [whole[near_rows], mirror[near_rows], whole[group + 8 * h : group + 8 * h + 8]]
            at = half + h * (group // 2)
            lower += [wrapped[near_rows], whole[at : at + group // 2]]
            lower += [whole[half + group + 8 * h : half + group + 8 * h + 8]]
        lower = jnp.concatenate(lower)
        if part == 1:
            lower = -lower
        both = jnp.concatenate([jnp.concatenate(upper), lower], axis=1)
        for k in range(0, order, half):
            folded[0, part, :, k : k + half] = dot(both, select[:, k : k + half]).astype(bf16)
    total = jnp.sum(jnp.sum(energy, axis=1, keepdims=True), axis=0, keepdims=True)
    factor[0] = jnp.broadcast_to(lax.rsqrt(total), factor.shape[1:])


def section_rows(folded, white, inverse, block, template, side, here, put):
    group = inverse.shape[1] // 2
    half = 2 * group
    cols = slice(side * half, (side + 1) * half)
    vr, vi = white[block, 0, :, cols], white[block, 1, :, cols]
    gr, gi = folded[template, 0, here, cols], folded[template, 1, here, cols]
    pr = gr * vr + gi * vi
    pi = gr * vi - gi * vr
    one, two = (
        dot(jnp.concatenate([pr[:, part], pi[:, part]], axis=1), inverse[group_order[2 * side + k]])
        for k, part in enumerate((slice(0, group), slice(group, half)))
    )
    plus, minus = one + two, one - two
    if side == 0:
        real, imag = (plus[:, :group], minus[:, :group]), (plus[:, group:], minus[:, group:])
    else:
        real, imag = (plus[:, :group], two[:, group:] - one[:, group:]), (plus[:, group:], minus[:, :group])
    put(2 * side, jnp.concatenate(real, axis=1).astype(bf16))
    put(2 * side + 1, jnp.concatenate(imag, axis=1).astype(bf16))


def fill_weights(pieces, weight, blocks):
    bank = lax.axis_index("bank")
    chunk = pieces.shape[1]
    for s in range(pieces.shape[0]):
        at = pl.multiple_of((bank ^ s) * chunk, 8)
        weight[pl.ds(at, chunk), :] = lax.rsqrt(pieces[s].astype(f32) / blocks + epsilon)


def whiten_rows(spectra, weight, white, block, side, here):
    chunk, half = white.shape[2], white.shape[3] // 2
    cols = slice(side * half, (side + 1) * half)
    tiles = range(side * half // 128, (side + 1) * half // 128)
    scale = jnp.concatenate([weight[t * chunk : (t + 1) * chunk, :] for t in tiles], axis=1)
    for part in range(2):
        white[block, part, :, cols] = (spectra[part, here, cols].astype(f32) * scale).astype(bf16)


def turned(sums, turn, at, size):
    span = slice(at, at + size)
    half = sums.shape[2]
    r0, i0, r1, i1 = (sums[plane, span] for plane in range(4))
    values = []
    for side, (ir, ii) in enumerate(((r0 + r1, i0 + i1), (r0 - r1, i0 - i1))):
        cols = slice(side * half, (side + 1) * half)
        tc, ts = turn[0, span, cols], turn[1, span, cols]
        values.append((ir * tc - ii * ts, ii * tc + ir * ts))
    return values


def twists(sums, turn, which, part, parts, put):
    half = sums.shape[2]
    near_count = half // 4
    step = 16
    first = (lax.broadcasted_iota(jnp.int32, (step, half), 0) == 0) & (which == 0)
    for at in range(part * near_count // parts, (part + 1) * near_count // parts, step):
        near_rows, far_rows = turned(sums, turn, at, step), turned(sums, turn, near_count + at, step)
        middle = turned(sums, turn, 2 * near_count, 8) if at == 0 else None
        for side in range(2):
            (r0, i0), (r1, i1) = near_rows[side], far_rows[side]
            for parity in range(2):
                re, im = (r0 + r1, i0 - i1) if parity == 0 else (r0 - r1, i0 + i1)
                if at == 0:
                    row = middle[side][parity][:1].astype(f32)
                    im = jnp.where(first, jnp.broadcast_to(row, im.shape), im.astype(f32)).astype(bf16)
                put(parity, side, at, re)
                put(parity, side, near_count + at, im)


def own_rows_kernel(
    mine, earlier, later, folded, twist, inverse, back, weight, white, turn, even_sums, odd_sums, *, blocks
):
    chunk, count = white.shape[2], folded.shape[0]
    core = lax.rem(lax.axis_index("tm"), 2)
    here = pl.ds(pl.multiple_of(core * chunk, 8), chunk)
    fill_weights(mine, weight, blocks)
    turn[...] = twist[:, here, :].astype(bf16)
    total = 2 * count
    for slot in range(total + 1):
        for j in range(2):
            if slot < total:
                block, template = divmod(slot, count)
                sums = (even_sums, odd_sums)[slot % 2]
                if template == 0:
                    whiten_rows((earlier, later)[block], weight, white, block, j, here)

                def put_sums(plane, value):
                    sums[plane] = value

                section_rows(folded, white, inverse, block, template, j, here, put_sums)
            if slot > 0:

                def put_back(parity, side, at, value):
                    back[slot - 1, parity, side, at : at + value.shape[0]] = value

                twists((even_sums, odd_sums)[(slot - 1) % 2], turn, core, j, 2, put_back)


def own_scratch(blocks, rows, order):
    half = order // 2
    return [
        pltpu.VMEM((rows // 2 * order // 128, 128), f32),
        pltpu.VMEM((blocks, 2, rows // 2, order), bf16),
        pltpu.VMEM((2, rows // 2, order), bf16),
        pltpu.VMEM((4, rows // 2, half), bf16),
        pltpu.VMEM((4, rows // 2, half), bf16),
    ]


def filter_scratch(blocks, count, rows, order):
    half, pairs = order // 2, blocks * count
    return own_scratch(blocks, rows, order) + [
        pltpu.VMEM((2, 2, half // 2, half), bf16),
        pltpu.VMEM((2, 2, half // 2, half), bf16),
        pltpu.VMEM((pairs, 2, half // 2, order), f32),
        pltpu.SemaphoreType.DMA((pairs,)),
    ]


def filter_kernel(
    theirs, own, earlier, later, folded, factor, twist, inverse, last, out,
    weight, white, turn, even_sums, odd_sums, even_back, odd_back, result, sems, *, blocks
):
    group = last.shape[2]
    half, order = 2 * group, 4 * group
    count, chunk = folded.shape[0], white.shape[2]
    lanes = order // 128
    core = lax.rem(lax.axis_index("tm"), 2)
    there = pl.ds(pl.multiple_of((1 - core) * chunk, 8), chunk)
    fill_weights(theirs, weight, blocks)
    turn[...] = twist[:, there, :].astype(bf16)

    def copies(slot):
        block, template = divmod(slot, count)
        return [
            pltpu.make_async_copy(
                result.at[slot, parity, :, pl.ds(lane * 128, 128)],
                out.at[pl.ds(block * group, group), parity, lane * count + template, 0, :],
                sems.at[slot],
            )
            for parity in range(2)
            for lane in range(lanes)
        ]

    def products(slot, side):
        block, template = divmod(slot, count)
        sums = (even_sums, odd_sums)[slot % 2]
        if template == 0:
            whiten_rows((earlier, later)[block], weight, white, block, side, there)

        def put(plane, value):
            sums[plane] = value

        section_rows(folded, white, inverse, block, template, side, there, put)

    def turns(slot, part):
        back = (even_back, odd_back)[slot % 2]

        def put(parity, side, at, value):
            back[parity, side, at : at + value.shape[0]] = value

        twists((even_sums, odd_sums)[slot % 2], turn, 1 - core, part, 2, put)

    def finish(slot, parity, side):
        back = (even_back, odd_back)[slot % 2]
        scale = factor[slot % count, 0:1, 0:1]
        whole = jnp.concatenate([own[slot, parity, side], back[parity, side]], axis=0)
        result[slot, parity, :, side * half : (side + 1) * half] = dot(last[parity, core], whole) * scale

    total = 2 * count
    for step in range(total + 2):
        for j in range(2):
            if 0 <= step - 1 < total:
                turns(step - 1, j)
            if 0 <= step - 2:
                finish(step - 2, j, 0)
                finish(step - 2, j, 1)
            if step < total:
                products(step, j)
        if step % 2 == 1 and step >= 3:
            for slot in (step - 3, step - 2):
                for copy in copies(slot):
                    copy.start()
    for slot in range(total):
        for copy in copies(slot):
            copy.wait()


def exchange(values, axis, pairs_of):
    size = lax.axis_size(axis)
    return lax.ppermute(values, axis, [(i, pairs_of(i)) for i in range(size)])


def near(value):
    return pltpu.with_memory_space_constraint(value, pltpu.VMEM)


def far(value):
    return pltpu.with_memory_space_constraint(value, pltpu.HBM)


def body(strain, lengths, templates):
    blocks_here, local = strain.shape
    count, order = templates.shape[1], templates.shape[-1]
    half = order // 2
    rows = half + 16
    banks, groups = lax.axis_size("bank"), lax.axis_size("tm")
    table = tables(order)
    vmem = pl.BlockSpec(memory_space=pltpu.VMEM)
    limit = pltpu.CompilerParams(vmem_limit_bytes=20 * 1024 * 1024)

    rowwise = jnp.swapaxes(strain.reshape(blocks_here, local // 128, 128), 0, 1)
    gated = pl.pallas_call(
        gate_kernel,
        in_specs=[pl.BlockSpec(memory_space=pltpu.SMEM), vmem],
        out_specs=vmem,
        out_shape=pltpu.VMEM((blocks_here, local // order, order), bf16),
        cost_estimate=pl.CostEstimate(flops=int(1e6), bytes_accessed=int(4e5), transcendentals=0),
        compiler_params=limit,
        name="gate",
    )(far(lengths), far(rowwise.reshape(blocks_here * local // 128, 128)))
    pieces = [gated] + [exchange(gated, "bank", lambda i, s=s: i ^ s) for s in range(1, banks)]

    folded, factor = pl.pallas_call(
        template_kernel,
        grid=(count,),
        in_specs=[pl.BlockSpec((2, 1, order, order), lambda t: (0, t, 0, 0))],
        out_specs=[
            pl.BlockSpec((1, 2, rows, order), lambda t: (t, 0, 0, 0)),
            pl.BlockSpec((1, 8, 128), lambda t: (t, 0, 0)),
        ],
        out_shape=[
            jax.ShapeDtypeStruct((count, 2, rows, order), bf16),
            jax.ShapeDtypeStruct((count, 8, 128), f32),
        ],
        scratch_shapes=[pltpu.VMEM((2 * order, order), bf16)],
        cost_estimate=pl.CostEstimate(flops=int(6e9), bytes_accessed=int(6.5e6), transcendentals=0),
        compiler_params=limit,
        name="fold_templates",
    )(far(templates))
    *pieces, factor = lax.optimization_barrier((*pieces, factor))

    plane = pltpu.VMEM((2, rows, order), bf16)
    chunk = rows * order // 128 // (2 * banks)
    kept, later, mine, other, last_block = pl.pallas_call(
        functools.partial(spectrum_kernel, shards=banks),
        in_specs=[vmem] * (banks + 3),
        out_specs=[vmem] * 5,
        out_shape=[plane, plane]
        + [pltpu.VMEM((chunk, 128), bf16)] * 2
        + [pltpu.VMEM((half, order), bf16)],
        scratch_shapes=[
            pltpu.VMEM((blocks_here, half, order), bf16),
            pltpu.VMEM((rows * order // 128, 128), f32),
        ],
        cost_estimate=pl.CostEstimate(flops=int(2e9), bytes_accessed=int(5e6), transcendentals=0),
        compiler_params=limit,
        name="spectra",
    )(*map(near, pieces), table["first"], table["twist"], table["forward"])

    partner = exchange(other, "tm", lambda i: i ^ 1)
    chip = (mine.astype(f32) + partner.astype(f32)).astype(bf16)
    share = chip.astype(f32)
    for step in range(1, groups // 2):
        share = share + exchange(chip, "tm", lambda i, s=step: i ^ (2 * s)).astype(f32)
    share = share.astype(bf16)

    before = lax.ppermute(last_block, "tm", [(i, (i + 1) % groups) for i in range(groups)])
    earlier = pl.pallas_call(
        previous_kernel,
        in_specs=[vmem] * 5,
        out_specs=vmem,
        out_shape=plane,
        cost_estimate=pl.CostEstimate(flops=int(1e9), bytes_accessed=int(4e6), transcendentals=0),
        compiler_params=limit,
        name="previous",
    )(near(before), near(kept), table["first"], table["twist"], table["forward"])

    shares = [share] + [exchange(share, "bank", lambda i, s=s: i ^ s) for s in range(1, banks)]
    *shares, earlier = lax.optimization_barrier((*shares, earlier))
    mine = jnp.stack(shares)
    theirs = exchange(mine, "tm", lambda i: i ^ 1)

    lanes = order // 128
    blocks = float(blocks_here * groups)
    own = pl.pallas_call(
        functools.partial(own_rows_kernel, blocks=blocks),
        in_specs=[vmem] * 6,
        out_specs=vmem,
        out_shape=pltpu.VMEM((blocks_here * count, 2, 2, half // 2, half), bf16),
        scratch_shapes=own_scratch(blocks_here, rows, order),
        cost_estimate=pl.CostEstimate(flops=int(2e9), bytes_accessed=int(6e6), transcendentals=0),
        compiler_params=limit,
        name="own_rows",
    )(near(mine), near(earlier), near(later), near(folded), table["twist"], table["inverse"])
    out = pl.pallas_call(
        functools.partial(filter_kernel, blocks=blocks),
        in_specs=[vmem] * 9,
        out_specs=pl.BlockSpec(memory_space=pl.ANY),
        out_shape=jax.ShapeDtypeStruct((blocks_here * half // 2, 2, lanes * count, 1, 128), f32),
        scratch_shapes=filter_scratch(blocks_here, count, rows, order),
        cost_estimate=pl.CostEstimate(flops=int(6e9), bytes_accessed=int(1.2e7), transcendentals=0),
        compiler_params=limit,
        name="filter",
    )(
        near(theirs), near(own), near(earlier), near(later), near(folded), near(factor),
        table["twist"], table["inverse"], table["last"],
    )
    split = out.reshape(blocks_here * half * lanes, count, 128)
    return jnp.swapaxes(split, 0, 1).reshape(count, blocks_here * half * order)


def solution(mesh):
    in_specs = (P("tm", "bank"), P("tm"), P(None, "bank", None, None))
    out_specs = P("bank", "tm")
    return jax.shard_map(body, mesh=mesh, in_specs=in_specs, out_specs=out_specs, check_vma=False)
```

```python
import functools
import math

import jax
import jax.numpy as jnp
import numpy as np
from jax import lax
from jax.experimental import pallas as pl
from jax.experimental.pallas import tpu as pltpu
from jax.sharding import PartitionSpec as P

epsilon = 1e-06
bf16 = jnp.bfloat16
f32 = jnp.float32
group_order = (0, 2, 1, 3)


def dot(a, b):
    return jnp.dot(a, b, preferred_element_type=f32)


def tables(order):
    half, group, eighth = order // 2, order // 4, order // 8
    i, pad = np.arange(group), np.zeros(8, np.int64)
    middle = np.concatenate([[group], pad[1:]])
    a = np.concatenate([i[:eighth], half - i[:eighth], middle, i[eighth:], half - i[eighth:], pad])
    rows = half + 16
    keep = np.ones((rows, 1))
    keep[group + 1 : group + 8] = 0
    keep[rows - 8 :] = 0
    turn = 2.0 * math.pi / order

    def angle(left, right):
        return turn * ((left[:, None] * right[None, :]) % order)

    u, v, g = np.arange(half), np.arange(order), np.arange(group)
    first = np.concatenate([np.cos(angle(a, u)) * keep, -np.sin(angle(a, u)) * keep])
    twist = (2.0 * math.pi / order**2) * (a[:, None] * v[None, :])
    forward, inverse = [], []
    for q in range(4):
        c, s = np.cos(angle(g, 4 * g + q)), np.sin(angle(g, 4 * g + q))
        forward.append(np.block([[c, -s], [s, c]]))
        inverse.append(np.block([[c.T, s.T], [-s.T, c.T]]))
    last = []
    for parity in range(2):
        w = 2 * g + parity
        c, s = np.cos(angle(w, g)), -np.sin(angle(w, g))
        c[:, 0] = 0.5
        s[:, 0] = (1.0 - 2.0 * parity) * (1.0 - 2.0 * (g % 2))
        sides = [np.concatenate([c[:, h], s[:, h]], axis=1) for h in (slice(0, eighth), slice(eighth, group))]
        last.append([np.concatenate([sides[core], sides[1 - core]], axis=1) for core in range(2)])
    return dict(
        first=first.astype(bf16),
        twist=np.stack([np.cos(twist), np.sin(twist)]).astype(np.float32),
        forward=np.stack(forward).astype(bf16),
        inverse=np.stack(inverse).astype(bf16),
        last=np.stack(last).astype(bf16),
    )


def gate_kernel(lengths, strain, gated):
    blocks, count, order = gated.shape
    lanes = order // 128
    start = lax.axis_index("bank") * (count * order)
    row = lax.broadcasted_iota(jnp.int32, (count, 128), 0)
    column = lax.broadcasted_iota(jnp.int32, (count, 128), 1)
    for block in range(blocks):
        for lane in range(lanes):
            x = strain[pl.ds(lane * blocks + block, count, stride=lanes * blocks), :]
            position = start + row * order + lane * 128 + column
            gated[block, :, lane * 128 : (lane + 1) * 128] = jnp.where(
                position < lengths[block], x, 0.0
            ).astype(bf16)


def quarters(value):
    group = value.shape[1] // 4
    return [value[:, q * group : (q + 1) * group] for q in range(4)]


def spectrum(samples, first, twist, forward):
    rows = first.shape[0] // 2
    out = dot(first[...], samples)
    real, imag = out[:rows], out[rows:]
    tc, ts = twist[0], twist[1]
    r = quarters(real * tc + imag * ts)
    i = quarters(imag * tc - real * ts)
    ar, ai, br, bi = r[0] + r[2], i[0] + i[2], r[1] + r[3], i[1] + i[3]
    cr, ci, dr, di = r[0] - r[2], i[0] - i[2], r[1] - r[3], i[1] - i[3]
    parts = [(ar + br, ai + bi), (cr + di, ci - dr), (ar - br, ai - bi), (cr - di, ci + dr)]
    return [
        dot(jnp.concatenate(part, axis=1).astype(bf16), forward[q]) for q, part in enumerate(parts)
    ]


def alternate(values):
    row = lax.broadcasted_iota(jnp.int32, values.shape, 0)
    return jnp.where(row % 2 == 0, values, -values)


def spectrum_kernel(*refs, shards):
    pieces = refs[:shards]
    first, twist, forward = refs[shards : shards + 3]
    kept, summed, mine, other, last_block, samples, power = refs[shards + 3 :]
    rows = first.shape[0] // 2
    group = forward.shape[1] // 2
    piece_rows = pieces[0].shape[1]
    bank, core = lax.axis_index("bank"), lax.rem(lax.axis_index("tm"), 2)
    for s in range(shards):
        at = pl.multiple_of((bank ^ s) * piece_rows, piece_rows)
        samples[:, pl.ds(at, piece_rows), :] = pieces[s][...]
    last_block[...] = samples[1]
    ones = spectrum(samples[0], first, twist, forward)
    twos = spectrum(samples[1], first, twist, forward)
    for place, q in enumerate(group_order):
        one, two = ones[q], twos[q]
        cols = slice(place * group, (place + 1) * group)
        for part in range(2):
            x0 = one[:, part * group : (part + 1) * group]
            x1 = two[:, part * group : (part + 1) * group]
            kept[part, :, cols] = x0.astype(bf16)
            summed[part, :, cols] = (x1 + alternate(x0)).astype(bf16)
        total = one * one + two * two
        total = total[:, :group] + total[:, group:]
        lanes = group // 128
        for lane in range(lanes):
            for h in range(2):
                row = (h * 4 * lanes + place * lanes + lane) * (rows // 2)
                piece = total[h * (rows // 2) : (h + 1) * (rows // 2), lane * 128 : (lane + 1) * 128]
                power[row : row + rows // 2, :] = piece
    chunk = mine.shape[0]
    for dest, which in ((mine, core), (other, 1 - core)):
        at = pl.multiple_of(which * (power.shape[0] // 2) + bank * chunk, 8)
        dest[...] = power[pl.ds(at, chunk), :].astype(bf16)


def previous_kernel(samples, kept, first, twist, forward, summed):
    group = forward.shape[1] // 2
    follows = lax.axis_index("tm") > 0
    parts = spectrum(jnp.where(follows, samples[...].astype(f32), 0.0).astype(bf16), first, twist, forward)
    for place, q in enumerate(group_order):
        x = parts[q]
        cols = slice(place * group, (place + 1) * group)
        for part in range(2):
            added = alternate(x[:, part * group : (part + 1) * group])
            summed[part, :, cols] = (kept[part, :, cols].astype(f32) + added).astype(bf16)


def template_kernel(templates, folded, factor, select):
    order = templates.shape[-1]
    half, group = order // 2, order // 4

    @pl.when(pl.program_id(0) == 0)
    def _():
        m = lax.broadcasted_iota(jnp.int32, (order, order), 0)
        n = lax.broadcasted_iota(jnp.int32, (order, order), 1)
        place = n // group
        source = 4 * (n % group) + jnp.where((place == 1) | (place == 2), 3 - place, place)
        select[:order] = jnp.where(m == source, 1.0, 0.0).astype(bf16)
        select[order:] = jnp.where(m == order - 1 - source, 1.0, 0.0).astype(bf16)

    i = lax.broadcasted_iota(jnp.int32, (group, group), 0)
    r = lax.broadcasted_iota(jnp.int32, (group, group), 1)
    flip = jnp.where(r == group - i, 1.0, 0.0).astype(bf16)
    start = lax.broadcasted_iota(jnp.int32, (group, order), 0) == 0
    energy = jnp.zeros((8, order), f32)
    for part in range(2):
        whole = templates[part, 0]
        wide = whole.astype(f32)
        energy = energy + jnp.sum((wide * wide).reshape(order // 8, 8, order), axis=0)

        def flipped(at, head):
            return jnp.where(start, head, dot(flip, whole[at : at + group])).astype(bf16)

        turned = pltpu.roll(wide[:8], order - 1, 1)[:1]
        mirror, wrapped = flipped(group, wide[half : half + 1]), flipped(half + group, turned)
        upper, lower = [], []
        for h in range(2):
            near_rows = slice(h * (group // 2), (h + 1) * (group // 2))
            upper += [whole[near_rows], mirror[near_rows], whole[group + 8 * h : group + 8 * h + 8]]
            at = half + h * (group // 2)
            lower += [wrapped[near_rows], whole[at : at + group // 2]]
            lower += [whole[half + group + 8 * h : half + group + 8 * h + 8]]
        lower = jnp.concatenate(lower)
        if part == 1:
            lower = -lower
        both = jnp.concatenate([jnp.concatenate(upper), lower], axis=1)
        for k in range(0, order, half):
            folded[0, part, :, k : k + half] = dot(both, select[:, k : k + half]).astype(bf16)
    total = jnp.sum(jnp.sum(energy, axis=1, keepdims=True), axis=0, keepdims=True)
    factor[0] = jnp.broadcast_to(lax.rsqrt(total), factor.shape[1:])


def section_rows(folded, white, inverse, block, template, side, here, put):
    group = inverse.shape[1] // 2
    half = 2 * group
    cols = slice(side * half, (side + 1) * half)
    vr, vi = white[block, 0, :, cols], white[block, 1, :, cols]
    gr, gi = folded[template, 0, here, cols], folded[template, 1, here, cols]
    pr = gr * vr + gi * vi
    pi = gr * vi - gi * vr
    one, two = (
        dot(jnp.concatenate([pr[:, part], pi[:, part]], axis=1), inverse[group_order[2 * side + k]])
        for k, part in enumerate((slice(0, group), slice(group, half)))
    )
    plus, minus = one + two, one - two
    if side == 0:
        real, imag = (plus[:, :group], minus[:, :group]), (plus[:, group:], minus[:, group:])
    else:
        real, imag = (plus[:, :group], two[:, group:] - one[:, group:]), (plus[:, group:], minus[:, :group])
    put(2 * side, jnp.concatenate(real, axis=1).astype(bf16))
    put(2 * side + 1, jnp.concatenate(imag, axis=1).astype(bf16))


def fill_weights(pieces, weight, blocks):
    bank = lax.axis_index("bank")
    chunk = pieces.shape[1]
    for s in range(pieces.shape[0]):
        at = pl.multiple_of((bank ^ s) * chunk, 8)
        weight[pl.ds(at, chunk), :] = lax.rsqrt(pieces[s].astype(f32) / blocks + epsilon)


def whiten_rows(spectra, weight, white, block, side, here):
    chunk, half = white.shape[2], white.shape[3] // 2
    cols = slice(side * half, (side + 1) * half)
    tiles = range(side * half // 128, (side + 1) * half // 128)
    scale = jnp.concatenate([weight[t * chunk : (t + 1) * chunk, :] for t in tiles], axis=1)
    for part in range(2):
        white[block, part, :, cols] = (spectra[part, here, cols].astype(f32) * scale).astype(bf16)


def turned(sums, turn, at, size):
    span = slice(at, at + size)
    half = sums.shape[2]
    r0, i0, r1, i1 = (sums[plane, span] for plane in range(4))
    values = []
    for side, (ir, ii) in enumerate(((r0 + r1, i0 + i1), (r0 - r1, i0 - i1))):
        cols = slice(side * half, (side + 1) * half)
        tc, ts = turn[0, span, cols], turn[1, span, cols]
        values.append((ir * tc - ii * ts, ii * tc + ir * ts))
    return values


def twists(sums, turn, which, part, parts, put):
    half = sums.shape[2]
    near_count = half // 4
    step = 16
    first = (lax.broadcasted_iota(jnp.int32, (step, half), 0) == 0) & (which == 0)
    for at in range(part * near_count // parts, (part + 1) * near_count // parts, step):
        near_rows, far_rows = turned(sums, turn, at, step), turned(sums, turn, near_count + at, step)
        middle = turned(sums, turn, 2 * near_count, 8) if at == 0 else None
        for side in range(2):
            (r0, i0), (r1, i1) = near_rows[side], far_rows[side]
            for parity in range(2):
                re, im = (r0 + r1, i0 - i1) if parity == 0 else (r0 - r1, i0 + i1)
                if at == 0:
                    row = middle[side][parity][:1].astype(f32)
                    im = jnp.where(first, jnp.broadcast_to(row, im.shape), im.astype(f32)).astype(bf16)
                put(parity, side, at, re)
                put(parity, side, near_count + at, im)


def own_rows_kernel(
    mine, earlier, later, folded, twist, inverse, back, weight, white, turn, even_sums, odd_sums, *, blocks
):
    chunk, count = white.shape[2], folded.shape[0]
    core = lax.rem(lax.axis_index("tm"), 2)
    here = pl.ds(pl.multiple_of(core * chunk, 8), chunk)
    fill_weights(mine, weight, blocks)
    turn[...] = twist[:, here, :].astype(bf16)
    total = 2 * count
    for slot in range(total + 1):
        for j in range(2):
            if slot < total:
                block, template = divmod(slot, count)
                sums = (even_sums, odd_sums)[slot % 2]
                if template == 0:
                    whiten_rows((earlier, later)[block], weight, white, block, j, here)

                def put_sums(plane, value):
                    sums[plane] = value

                section_rows(folded, white, inverse, block, template, j, here, put_sums)
            if slot > 0:

                def put_back(parity, side, at, value):
                    back[slot - 1, parity, side, at : at + value.shape[0]] = value

                twists((even_sums, odd_sums)[(slot - 1) % 2], turn, core, j, 2, put_back)


def own_scratch(blocks, rows, order):
    half = order // 2
    return [
        pltpu.VMEM((rows // 2 * order // 128, 128), f32),
        pltpu.VMEM((blocks, 2, rows // 2, order), bf16),
        pltpu.VMEM((2, rows // 2, order), bf16),
        pltpu.VMEM((4, rows // 2, half), bf16),
        pltpu.VMEM((4, rows // 2, half), bf16),
    ]


def filter_scratch(blocks, count, rows, order):
    half, pairs = order // 2, blocks * count
    return own_scratch(blocks, rows, order) + [
        pltpu.VMEM((2, 2, half // 2, half), bf16),
        pltpu.VMEM((2, 2, half // 2, half), bf16),
        pltpu.VMEM((pairs, 2, half // 2, order), f32),
        pltpu.SemaphoreType.DMA((pairs,)),
    ]


def filter_kernel(
    theirs, own, earlier, later, folded, factor, twist, inverse, last, out,
    weight, white, turn, even_sums, odd_sums, even_back, odd_back, result, sems, *, blocks
):
    group = last.shape[2]
    half, order = 2 * group, 4 * group
    count, chunk = folded.shape[0], white.shape[2]
    lanes = order // 128
    core = lax.rem(lax.axis_index("tm"), 2)
    there = pl.ds(pl.multiple_of((1 - core) * chunk, 8), chunk)
    fill_weights(theirs, weight, blocks)
    turn[...] = twist[:, there, :].astype(bf16)

    def copies(slot):
        block, template = divmod(slot, count)
        return [
            pltpu.make_async_copy(
                result.at[slot, parity, :, pl.ds(lane * 128, 128)],
                out.at[pl.ds(block * group, group), parity, lane * count + template, 0, :],
                sems.at[slot],
            )
            for parity in range(2)
            for lane in range(lanes)
        ]

    def products(slot, side):
        block, template = divmod(slot, count)
        sums = (even_sums, odd_sums)[slot % 2]
        if template == 0:
            whiten_rows((earlier, later)[block], weight, white, block, side, there)

        def put(plane, value):
            sums[plane] = value

        section_rows(folded, white, inverse, block, template, side, there, put)

    def turns(slot, part):
        back = (even_back, odd_back)[slot % 2]

        def put(parity, side, at, value):
            back[parity, side, at : at + value.shape[0]] = value

        twists((even_sums, odd_sums)[slot % 2], turn, 1 - core, part, 2, put)

    def finish(slot, parity, side):
        back = (even_back, odd_back)[slot % 2]
        scale = factor[slot % count, 0:1, 0:1]
        whole = jnp.concatenate([own[slot, parity, side], back[parity, side]], axis=0)
        result[slot, parity, :, side * half : (side + 1) * half] = dot(last[parity, core], whole) * scale

    total = 2 * count
    for step in range(total + 2):
        for j in range(2):
            if 0 <= step - 1 < total:
                turns(step - 1, j)
            if 0 <= step - 2:
                finish(step - 2, j, 0)
                finish(step - 2, j, 1)
            if step < total:
                products(step, j)
        if step % 2 == 1 and step >= 3:
            for slot in (step - 3, step - 2):
                for copy in copies(slot):
                    copy.start()
    for slot in range(total):
        for copy in copies(slot):
            copy.wait()


def exchange(values, axis, pairs_of):
    size = lax.axis_size(axis)
    return lax.ppermute(values, axis, [(i, pairs_of(i)) for i in range(size)])


def near(value):
    return pltpu.with_memory_space_constraint(value, pltpu.VMEM)


def far(value):
    return pltpu.with_memory_space_constraint(value, pltpu.HBM)


def body(strain, lengths, templates):
    blocks_here, local = strain.shape
    count, order = templates.shape[1], templates.shape[-1]
    half = order // 2
    rows = half + 16
    banks, groups = lax.axis_size("bank"), lax.axis_size("tm")
    table = tables(order)
    vmem = pl.BlockSpec(memory_space=pltpu.VMEM)
    limit = pltpu.CompilerParams(vmem_limit_bytes=20 * 1024 * 1024)

    rowwise = jnp.swapaxes(strain.reshape(blocks_here, local // 128, 128), 0, 1)
    gated = pl.pallas_call(
        gate_kernel,
        in_specs=[pl.BlockSpec(memory_space=pltpu.SMEM), vmem],
        out_specs=vmem,
        out_shape=pltpu.VMEM((blocks_here, local // order, order), bf16),
        cost_estimate=pl.CostEstimate(flops=int(1e6), bytes_accessed=int(4e5), transcendentals=0),
        compiler_params=limit,
        name="gate",
    )(far(lengths), far(rowwise.reshape(blocks_here * local // 128, 128)))
    pieces = [gated] + [exchange(gated, "bank", lambda i, s=s: i ^ s) for s in range(1, banks)]

    folded, factor = pl.pallas_call(
        template_kernel,
        grid=(count,),
        in_specs=[pl.BlockSpec((2, 1, order, order), lambda t: (0, t, 0, 0))],
        out_specs=[
            pl.BlockSpec((1, 2, rows, order), lambda t: (t, 0, 0, 0)),
            pl.BlockSpec((1, 8, 128), lambda t: (t, 0, 0)),
        ],
        out_shape=[
            jax.ShapeDtypeStruct((count, 2, rows, order), bf16),
            jax.ShapeDtypeStruct((count, 8, 128), f32),
        ],
        scratch_shapes=[pltpu.VMEM((2 * order, order), bf16)],
        cost_estimate=pl.CostEstimate(flops=int(6e9), bytes_accessed=int(6.5e6), transcendentals=0),
        compiler_params=limit,
        name="fold_templates",
    )(far(templates))
    *pieces, factor = lax.optimization_barrier((*pieces, factor))

    plane = pltpu.VMEM((2, rows, order), bf16)
    chunk = rows * order // 128 // (2 * banks)
    kept, later, mine, other, last_block = pl.pallas_call(
        functools.partial(spectrum_kernel, shards=banks),
        in_specs=[vmem] * (banks + 3),
        out_specs=[vmem] * 5,
        out_shape=[plane, plane]
        + [pltpu.VMEM((chunk, 128), bf16)] * 2
        + [pltpu.VMEM((half, order), bf16)],
        scratch_shapes=[
            pltpu.VMEM((blocks_here, half, order), bf16),
            pltpu.VMEM((rows * order // 128, 128), f32),
        ],
        cost_estimate=pl.CostEstimate(flops=int(2e9), bytes_accessed=int(5e6), transcendentals=0),
        compiler_params=limit,
        name="spectra",
    )(*map(near, pieces), table["first"], table["twist"], table["forward"])

    partner = exchange(other, "tm", lambda i: i ^ 1)
    chip = (mine.astype(f32) + partner.astype(f32)).astype(bf16)
    share = chip.astype(f32)
    for step in sorted(range(1, groups // 2), key=lambda d: (d ^ 1) if d > 1 else d):
        share = share + exchange(chip, "tm", lambda i, s=step: i ^ (2 * s)).astype(f32)
    share = share.astype(bf16)

    before = lax.ppermute(last_block, "tm", [(i, (i + 1) % groups) for i in range(groups)])
    earlier = pl.pallas_call(
        previous_kernel,
        in_specs=[vmem] * 5,
        out_specs=vmem,
        out_shape=plane,
        cost_estimate=pl.CostEstimate(flops=int(1e9), bytes_accessed=int(4e6), transcendentals=0),
        compiler_params=limit,
        name="previous",
    )(near(before), near(kept), table["first"], table["twist"], table["forward"])

    shares = [share] + [exchange(share, "bank", lambda i, s=s: i ^ s) for s in range(1, banks)]
    *shares, earlier = lax.optimization_barrier((*shares, earlier))
    mine = jnp.stack(shares)
    theirs = exchange(mine, "tm", lambda i: i ^ 1)

    lanes = order // 128
    blocks = float(blocks_here * groups)
    own = pl.pallas_call(
        functools.partial(own_rows_kernel, blocks=blocks),
        in_specs=[vmem] * 6,
        out_specs=vmem,
        out_shape=pltpu.VMEM((blocks_here * count, 2, 2, half // 2, half), bf16),
        scratch_shapes=own_scratch(blocks_here, rows, order),
        cost_estimate=pl.CostEstimate(flops=int(2e9), bytes_accessed=int(6e6), transcendentals=0),
        compiler_params=limit,
        name="own_rows",
    )(near(mine), near(earlier), near(later), near(folded), table["twist"], table["inverse"])
    out = pl.pallas_call(
        functools.partial(filter_kernel, blocks=blocks),
        in_specs=[vmem] * 9,
        out_specs=pl.BlockSpec(memory_space=pl.ANY),
        out_shape=jax.ShapeDtypeStruct((blocks_here * half // 2, 2, lanes * count, 1, 128), f32),
        scratch_shapes=filter_scratch(blocks_here, count, rows, order),
        cost_estimate=pl.CostEstimate(flops=int(6e9), bytes_accessed=int(1.2e7), transcendentals=0),
        compiler_params=limit,
        name="filter",
    )(
        near(theirs), near(own), near(earlier), near(later), near(folded), near(factor),
        table["twist"], table["inverse"], table["last"],
    )
    split = out.reshape(blocks_here * half * lanes, count, 128)
    return jnp.swapaxes(split, 0, 1).reshape(count, blocks_here * half * order)


def solution(mesh):
    in_specs = (P("tm", "bank"), P("tm"), P(None, "bank", None, None))
    out_specs = P("bank", "tm")
    return jax.shard_map(body, mesh=mesh, in_specs=in_specs, out_specs=out_specs, check_vma=False)
```

```python
import functools
import math

import jax
import jax.numpy as jnp
import numpy as np
from jax import lax
from jax.experimental import pallas as pl
from jax.experimental.pallas import tpu as pltpu
from jax.sharding import PartitionSpec as P

epsilon = 1e-06
bf16 = jnp.bfloat16
f32 = jnp.float32
group_order = (0, 2, 1, 3)


def dot(a, b):
    return jnp.dot(a, b, preferred_element_type=f32)


def tables(order):
    half, group, eighth = order // 2, order // 4, order // 8
    i, pad = np.arange(group), np.zeros(8, np.int64)
    middle = np.concatenate([[group], pad[1:]])
    a = np.concatenate([i[:eighth], half - i[:eighth], middle, i[eighth:], half - i[eighth:], pad])
    rows = half + 16
    keep = np.ones((rows, 1))
    keep[group + 1 : group + 8] = 0
    keep[rows - 8 :] = 0
    turn = 2.0 * math.pi / order

    def angle(left, right):
        return turn * ((left[:, None] * right[None, :]) % order)

    u, v, g = np.arange(half), np.arange(order), np.arange(group)
    first = np.concatenate([np.cos(angle(a, u)) * keep, -np.sin(angle(a, u)) * keep])
    twist = (2.0 * math.pi / order**2) * (a[:, None] * v[None, :])
    forward, inverse = [], []
    for q in range(4):
        c, s = np.cos(angle(g, 4 * g + q)), np.sin(angle(g, 4 * g + q))
        forward.append(np.block([[c, -s], [s, c]]))
        inverse.append(np.block([[c.T, s.T], [-s.T, c.T]]))
    last = []
    for parity in range(2):
        w = 2 * g + parity
        c, s = np.cos(angle(w, g)), -np.sin(angle(w, g))
        c[:, 0] = 0.5
        s[:, 0] = (1.0 - 2.0 * parity) * (1.0 - 2.0 * (g % 2))
        sides = [np.concatenate([c[:, h], s[:, h]], axis=1) for h in (slice(0, eighth), slice(eighth, group))]
        last.append([np.concatenate([sides[core], sides[1 - core]], axis=1) for core in range(2)])
    return dict(
        first=first.astype(bf16),
        twist=np.stack([np.cos(twist), np.sin(twist)]).astype(np.float32),
        forward=np.stack(forward).astype(bf16),
        inverse=np.stack(inverse).astype(bf16),
        last=np.stack(last).astype(bf16),
    )


def gate_kernel(lengths, strain, gated):
    blocks, count, order = gated.shape
    lanes = order // 128
    start = lax.axis_index("bank") * (count * order)
    row = lax.broadcasted_iota(jnp.int32, (count, 128), 0)
    column = lax.broadcasted_iota(jnp.int32, (count, 128), 1)
    for block in range(blocks):
        for lane in range(lanes):
            x = strain[pl.ds(lane * blocks + block, count, stride=lanes * blocks), :]
            position = start + row * order + lane * 128 + column
            gated[block, :, lane * 128 : (lane + 1) * 128] = jnp.where(
                position < lengths[block], x, 0.0
            ).astype(bf16)


def quarters(value):
    group = value.shape[1] // 4
    return [value[:, q * group : (q + 1) * group] for q in range(4)]


def spectrum(samples, first, twist, forward):
    rows = first.shape[0] // 2
    out = dot(first[...], samples)
    real, imag = out[:rows], out[rows:]
    tc, ts = twist[0], twist[1]
    r = quarters(real * tc + imag * ts)
    i = quarters(imag * tc - real * ts)
    ar, ai, br, bi = r[0] + r[2], i[0] + i[2], r[1] + r[3], i[1] + i[3]
    cr, ci, dr, di = r[0] - r[2], i[0] - i[2], r[1] - r[3], i[1] - i[3]
    parts = [(ar + br, ai + bi), (cr + di, ci - dr), (ar - br, ai - bi), (cr - di, ci + dr)]
    return [
        dot(jnp.concatenate(part, axis=1).astype(bf16), forward[q]) for q, part in enumerate(parts)
    ]


def alternate(values):
    row = lax.broadcasted_iota(jnp.int32, values.shape, 0)
    return jnp.where(row % 2 == 0, values, -values)


def spectrum_kernel(*refs, shards):
    pieces = refs[:shards]
    first, twist, forward = refs[shards : shards + 3]
    kept, summed, mine, other, last_block, samples, power = refs[shards + 3 :]
    rows = first.shape[0] // 2
    group = forward.shape[1] // 2
    piece_rows = pieces[0].shape[1]
    bank, core = lax.axis_index("bank"), lax.rem(lax.axis_index("tm"), 2)
    for s in range(shards):
        at = pl.multiple_of((bank ^ s) * piece_rows, piece_rows)
        samples[:, pl.ds(at, piece_rows), :] = pieces[s][...]
    last_block[...] = samples[1]
    ones = spectrum(samples[0], first, twist, forward)
    twos = spectrum(samples[1], first, twist, forward)
    for place, q in enumerate(group_order):
        one, two = ones[q], twos[q]
        cols = slice(place * group, (place + 1) * group)
        for part in range(2):
            x0 = one[:, part * group : (part + 1) * group]
            x1 = two[:, part * group : (part + 1) * group]
            kept[part, :, cols] = x0.astype(bf16)
            summed[part, :, cols] = (x1 + alternate(x0)).astype(bf16)
        total = one * one + two * two
        total = total[:, :group] + total[:, group:]
        lanes = group // 128
        for lane in range(lanes):
            for h in range(2):
                row = (h * 4 * lanes + place * lanes + lane) * (rows // 2)
                piece = total[h * (rows // 2) : (h + 1) * (rows // 2), lane * 128 : (lane + 1) * 128]
                power[row : row + rows // 2, :] = piece
    chunk = mine.shape[0]
    for dest, which in ((mine, core), (other, 1 - core)):
        at = pl.multiple_of(which * (power.shape[0] // 2) + bank * chunk, 8)
        dest[...] = power[pl.ds(at, chunk), :].astype(bf16)


def previous_kernel(samples, kept, first, twist, forward, summed, narrow):
    narrow[...] = twist[...].astype(bf16)
    group = forward.shape[1] // 2
    follows = lax.axis_index("tm") > 0
    parts = spectrum(jnp.where(follows, samples[...].astype(f32), 0.0).astype(bf16), first, twist, forward)
    for place, q in enumerate(group_order):
        x = parts[q]
        cols = slice(place * group, (place + 1) * group)
        for part in range(2):
            added = alternate(x[:, part * group : (part + 1) * group])
            summed[part, :, cols] = (kept[part, :, cols].astype(f32) + added).astype(bf16)


def template_kernel(templates, folded, factor, select):
    order = templates.shape[-1]
    half, group = order // 2, order // 4

    @pl.when(pl.program_id(0) == 0)
    def _():
        m = lax.broadcasted_iota(jnp.int32, (order, order), 0)
        n = lax.broadcasted_iota(jnp.int32, (order, order), 1)
        place = n // group
        source = 4 * (n % group) + jnp.where((place == 1) | (place == 2), 3 - place, place)
        select[:order] = jnp.where(m == source, 1.0, 0.0).astype(bf16)
        select[order:] = jnp.where(m == order - 1 - source, 1.0, 0.0).astype(bf16)

    i = lax.broadcasted_iota(jnp.int32, (group, group), 0)
    r = lax.broadcasted_iota(jnp.int32, (group, group), 1)
    flip = jnp.where(r == group - i, 1.0, 0.0).astype(bf16)
    start = lax.broadcasted_iota(jnp.int32, (group, order), 0) == 0
    energy = jnp.zeros((8, order), f32)
    for part in range(2):
        whole = templates[part, 0]
        wide = whole.astype(f32)
        energy = energy + jnp.sum((wide * wide).reshape(order // 8, 8, order), axis=0)

        def flipped(at, head):
            return jnp.where(start, head, dot(flip, whole[at : at + group])).astype(bf16)

        turned = pltpu.roll(wide[:8], order - 1, 1)[:1]
        mirror, wrapped = flipped(group, wide[half : half + 1]), flipped(half + group, turned)
        upper, lower = [], []
        for h in range(2):
            near_rows = slice(h * (group // 2), (h + 1) * (group // 2))
            upper += [whole[near_rows], mirror[near_rows], whole[group + 8 * h : group + 8 * h + 8]]
            at = half + h * (group // 2)
            lower += [wrapped[near_rows], whole[at : at + group // 2]]
            lower += [whole[half + group + 8 * h : half + group + 8 * h + 8]]
        lower = jnp.concatenate(lower)
        if part == 1:
            lower = -lower
        both = jnp.concatenate([jnp.concatenate(upper), lower], axis=1)
        for k in range(0, order, half):
            folded[0, part, :, k : k + half] = dot(both, select[:, k : k + half]).astype(bf16)
    total = jnp.sum(jnp.sum(energy, axis=1, keepdims=True), axis=0, keepdims=True)
    factor[0] = jnp.broadcast_to(lax.rsqrt(total), factor.shape[1:])


def section_rows(folded, white, inverse, block, template, side, here, put):
    group = inverse.shape[1] // 2
    half = 2 * group
    cols = slice(side * half, (side + 1) * half)
    vr, vi = white[block, 0, :, cols], white[block, 1, :, cols]
    gr, gi = folded[template, 0, here, cols], folded[template, 1, here, cols]
    pr = gr * vr + gi * vi
    pi = gr * vi - gi * vr
    one, two = (
        dot(jnp.concatenate([pr[:, part], pi[:, part]], axis=1), inverse[group_order[2 * side + k]])
        for k, part in enumerate((slice(0, group), slice(group, half)))
    )
    plus, minus = one + two, one - two
    if side == 0:
        real, imag = (plus[:, :group], minus[:, :group]), (plus[:, group:], minus[:, group:])
    else:
        real, imag = (plus[:, :group], two[:, group:] - one[:, group:]), (plus[:, group:], minus[:, :group])
    put(2 * side, jnp.concatenate(real, axis=1).astype(bf16))
    put(2 * side + 1, jnp.concatenate(imag, axis=1).astype(bf16))


def fill_weights(pieces, weight, blocks):
    bank = lax.axis_index("bank")
    chunk = pieces.shape[1]
    for s in range(pieces.shape[0]):
        at = pl.multiple_of((bank ^ s) * chunk, 8)
        weight[pl.ds(at, chunk), :] = lax.rsqrt(pieces[s].astype(f32) / blocks + epsilon)


def whiten_rows(spectra, weight, white, block, side, here):
    chunk, half = white.shape[2], white.shape[3] // 2
    cols = slice(side * half, (side + 1) * half)
    tiles = range(side * half // 128, (side + 1) * half // 128)
    scale = jnp.concatenate([weight[t * chunk : (t + 1) * chunk, :] for t in tiles], axis=1)
    for part in range(2):
        white[block, part, :, cols] = (spectra[part, here, cols].astype(f32) * scale).astype(bf16)


def turned(sums, turn, at, size):
    span = slice(at, at + size)
    half = sums.shape[2]
    r0, i0, r1, i1 = (sums[plane, span] for plane in range(4))
    values = []
    for side, (ir, ii) in enumerate(((r0 + r1, i0 + i1), (r0 - r1, i0 - i1))):
        cols = slice(side * half, (side + 1) * half)
        tc, ts = turn[0, span, cols], turn[1, span, cols]
        values.append((ir * tc - ii * ts, ii * tc + ir * ts))
    return values


def twists(sums, turn, which, part, parts, put):
    half = sums.shape[2]
    near_count = half // 4
    step = 16
    first = (lax.broadcasted_iota(jnp.int32, (step, half), 0) == 0) & (which == 0)
    for at in range(part * near_count // parts, (part + 1) * near_count // parts, step):
        near_rows, far_rows = turned(sums, turn, at, step), turned(sums, turn, near_count + at, step)
        middle = turned(sums, turn, 2 * near_count, 8) if at == 0 else None
        for side in range(2):
            (r0, i0), (r1, i1) = near_rows[side], far_rows[side]
            for parity in range(2):
                re, im = (r0 + r1, i0 - i1) if parity == 0 else (r0 - r1, i0 + i1)
                if at == 0:
                    row = middle[side][parity][:1].astype(f32)
                    im = jnp.where(first, jnp.broadcast_to(row, im.shape), im.astype(f32)).astype(bf16)
                put(parity, side, at, re)
                put(parity, side, near_count + at, im)


def own_rows_kernel(
    mine, earlier, later, folded, twist, inverse, back, weight, white, even_sums, odd_sums, *, blocks
):
    chunk, count = white.shape[2], folded.shape[0]
    core = lax.rem(lax.axis_index("tm"), 2)
    here = pl.ds(pl.multiple_of(core * chunk, 8), chunk)
    fill_weights(mine, weight, blocks)
    turn = twist.at[:, here]
    total = 2 * count
    for slot in range(total + 1):
        for j in range(2):
            if slot < total:
                block, template = divmod(slot, count)
                sums = (even_sums, odd_sums)[slot % 2]
                if template == 0:
                    whiten_rows((earlier, later)[block], weight, white, block, j, here)

                def put_sums(plane, value):
                    sums[plane] = value

                section_rows(folded, white, inverse, block, template, j, here, put_sums)
            if slot > 0:

                def put_back(parity, side, at, value):
                    back[slot - 1, parity, side, at : at + value.shape[0]] = value

                twists((even_sums, odd_sums)[(slot - 1) % 2], turn, core, j, 2, put_back)


def own_scratch(blocks, rows, order):
    half = order // 2
    return [
        pltpu.VMEM((rows // 2 * order // 128, 128), f32),
        pltpu.VMEM((blocks, 2, rows // 2, order), bf16),
        pltpu.VMEM((4, rows // 2, half), bf16),
        pltpu.VMEM((4, rows // 2, half), bf16),
    ]


def filter_scratch(blocks, count, rows, order):
    half, pairs = order // 2, blocks * count
    return own_scratch(blocks, rows, order) + [
        pltpu.VMEM((2, 2, half // 2, half), bf16),
        pltpu.VMEM((2, 2, half // 2, half), bf16),
        pltpu.VMEM((pairs, 2, half // 2, order), f32),
        pltpu.SemaphoreType.DMA((pairs,)),
    ]


def filter_kernel(
    theirs, own, earlier, later, folded, factor, twist, inverse, last, out,
    weight, white, even_sums, odd_sums, even_back, odd_back, result, sems, *, blocks
):
    group = last.shape[2]
    half, order = 2 * group, 4 * group
    count, chunk = folded.shape[0], white.shape[2]
    lanes = order // 128
    core = lax.rem(lax.axis_index("tm"), 2)
    there = pl.ds(pl.multiple_of((1 - core) * chunk, 8), chunk)
    fill_weights(theirs, weight, blocks)
    turn = twist.at[:, there]

    def copies(slot):
        block, template = divmod(slot, count)
        return [
            pltpu.make_async_copy(
                result.at[slot, parity, :, pl.ds(lane * 128, 128)],
                out.at[pl.ds(block * group, group), parity, lane * count + template, 0, :],
                sems.at[slot],
            )
            for parity in range(2)
            for lane in range(lanes)
        ]

    def products(slot, side):
        block, template = divmod(slot, count)
        sums = (even_sums, odd_sums)[slot % 2]
        if template == 0:
            whiten_rows((earlier, later)[block], weight, white, block, side, there)

        def put(plane, value):
            sums[plane] = value

        section_rows(folded, white, inverse, block, template, side, there, put)

    def turns(slot, part):
        back = (even_back, odd_back)[slot % 2]

        def put(parity, side, at, value):
            back[parity, side, at : at + value.shape[0]] = value

        twists((even_sums, odd_sums)[slot % 2], turn, 1 - core, part, 2, put)

    def finish(slot, parity, side):
        back = (even_back, odd_back)[slot % 2]
        scale = factor[slot % count, 0:1, 0:1]
        whole = jnp.concatenate([own[slot, parity, side], back[parity, side]], axis=0)
        result[slot, parity, :, side * half : (side + 1) * half] = dot(last[parity, core], whole) * scale

    total = 2 * count
    for step in range(total + 2):
        for j in range(2):
            if 0 <= step - 1 < total:
                turns(step - 1, j)
            if 0 <= step - 2:
                finish(step - 2, j, 0)
                finish(step - 2, j, 1)
            if step < total:
                products(step, j)
        if step % 2 == 1 and step >= 3:
            for slot in (step - 3, step - 2):
                for copy in copies(slot):
                    copy.start()
    for slot in range(total):
        for copy in copies(slot):
            copy.wait()


def exchange(values, axis, pairs_of):
    size = lax.axis_size(axis)
    return lax.ppermute(values, axis, [(i, pairs_of(i)) for i in range(size)])


def near(value):
    return pltpu.with_memory_space_constraint(value, pltpu.VMEM)


def far(value):
    return pltpu.with_memory_space_constraint(value, pltpu.HBM)


def body(strain, lengths, templates):
    blocks_here, local = strain.shape
    count, order = templates.shape[1], templates.shape[-1]
    half = order // 2
    rows = half + 16
    banks, groups = lax.axis_size("bank"), lax.axis_size("tm")
    table = tables(order)
    vmem = pl.BlockSpec(memory_space=pltpu.VMEM)
    limit = pltpu.CompilerParams(vmem_limit_bytes=20 * 1024 * 1024)

    rowwise = jnp.swapaxes(strain.reshape(blocks_here, local // 128, 128), 0, 1)
    gated = pl.pallas_call(
        gate_kernel,
        in_specs=[pl.BlockSpec(memory_space=pltpu.SMEM), vmem],
        out_specs=vmem,
        out_shape=pltpu.VMEM((blocks_here, local // order, order), bf16),
        cost_estimate=pl.CostEstimate(flops=int(1e6), bytes_accessed=int(4e5), transcendentals=0),
        compiler_params=limit,
        name="gate",
    )(far(lengths), far(rowwise.reshape(blocks_here * local // 128, 128)))
    pieces = [gated] + [exchange(gated, "bank", lambda i, s=s: i ^ s) for s in range(1, banks)]

    folded, factor = pl.pallas_call(
        template_kernel,
        grid=(count,),
        in_specs=[pl.BlockSpec((2, 1, order, order), lambda t: (0, t, 0, 0))],
        out_specs=[
            pl.BlockSpec((1, 2, rows, order), lambda t: (t, 0, 0, 0)),
            pl.BlockSpec((1, 8, 128), lambda t: (t, 0, 0)),
        ],
        out_shape=[
            jax.ShapeDtypeStruct((count, 2, rows, order), bf16),
            jax.ShapeDtypeStruct((count, 8, 128), f32),
        ],
        scratch_shapes=[pltpu.VMEM((2 * order, order), bf16)],
        cost_estimate=pl.CostEstimate(flops=int(6e9), bytes_accessed=int(6.5e6), transcendentals=0),
        compiler_params=limit,
        name="fold_templates",
    )(far(templates))
    *pieces, factor = lax.optimization_barrier((*pieces, factor))

    plane = pltpu.VMEM((2, rows, order), bf16)
    chunk = rows * order // 128 // (2 * banks)
    kept, later, mine, other, last_block = pl.pallas_call(
        functools.partial(spectrum_kernel, shards=banks),
        in_specs=[vmem] * (banks + 3),
        out_specs=[vmem] * 5,
        out_shape=[plane, plane]
        + [pltpu.VMEM((chunk, 128), bf16)] * 2
        + [pltpu.VMEM((half, order), bf16)],
        scratch_shapes=[
            pltpu.VMEM((blocks_here, half, order), bf16),
            pltpu.VMEM((rows * order // 128, 128), f32),
        ],
        cost_estimate=pl.CostEstimate(flops=int(2e9), bytes_accessed=int(5e6), transcendentals=0),
        compiler_params=limit,
        name="spectra",
    )(*map(near, pieces), table["first"], table["twist"], table["forward"])

    partner = exchange(other, "tm", lambda i: i ^ 1)
    chip = (mine.astype(f32) + partner.astype(f32)).astype(bf16)
    share = chip.astype(f32)
    for step in sorted(range(1, groups // 2), key=lambda d: (d ^ 1) if d > 1 else d):
        share = share + exchange(chip, "tm", lambda i, s=step: i ^ (2 * s)).astype(f32)
    share = share.astype(bf16)

    before = lax.ppermute(last_block, "tm", [(i, (i + 1) % groups) for i in range(groups)])
    earlier, narrow = pl.pallas_call(
        previous_kernel,
        in_specs=[vmem] * 5,
        out_specs=[vmem] * 2,
        out_shape=[plane, plane],
        cost_estimate=pl.CostEstimate(flops=int(1e9), bytes_accessed=int(4e6), transcendentals=0),
        compiler_params=limit,
        name="previous",
    )(near(before), near(kept), table["first"], table["twist"], table["forward"])

    shares = [share] + [exchange(share, "bank", lambda i, s=s: i ^ s) for s in range(1, banks)]
    *shares, earlier = lax.optimization_barrier((*shares, earlier))
    mine = jnp.stack(shares)
    theirs = exchange(mine, "tm", lambda i: i ^ 1)

    lanes = order // 128
    blocks = float(blocks_here * groups)
    own = pl.pallas_call(
        functools.partial(own_rows_kernel, blocks=blocks),
        in_specs=[vmem] * 6,
        out_specs=vmem,
        out_shape=pltpu.VMEM((blocks_here * count, 2, 2, half // 2, half), bf16),
        scratch_shapes=own_scratch(blocks_here, rows, order),
        cost_estimate=pl.CostEstimate(flops=int(2e9), bytes_accessed=int(6e6), transcendentals=0),
        compiler_params=limit,
        name="own_rows",
    )(near(mine), near(earlier), near(later), near(folded), near(narrow), table["inverse"])
    out = pl.pallas_call(
        functools.partial(filter_kernel, blocks=blocks),
        in_specs=[vmem] * 9,
        out_specs=pl.BlockSpec(memory_space=pl.ANY),
        out_shape=jax.ShapeDtypeStruct((blocks_here * half // 2, 2, lanes * count, 1, 128), f32),
        scratch_shapes=filter_scratch(blocks_here, count, rows, order),
        cost_estimate=pl.CostEstimate(flops=int(6e9), bytes_accessed=int(1.2e7), transcendentals=0),
        compiler_params=limit,
        name="filter",
    )(
        near(theirs), near(own), near(earlier), near(later), near(folded), near(factor),
        near(narrow), table["inverse"], table["last"],
    )
    split = out.reshape(blocks_here * half * lanes, count, 128)
    return jnp.swapaxes(split, 0, 1).reshape(count, blocks_here * half * order)


def solution(mesh):
    in_specs = (P("tm", "bank"), P("tm"), P(None, "bank", None, None))
    out_specs = P("bank", "tm")
    return jax.shard_map(body, mesh=mesh, in_specs=in_specs, out_specs=out_specs, check_vma=False)
```
